128 devices in a mesh: rows: 16 (over z_lo, y, core), width: 8 (over z_hi, x).
Axes of the slice: x: 4, y: 4, z: 4 (z_hi: 2, z_lo: 2; z = z_hi * 2 + z_lo), core: 2. Of those that a mesh axis runs over, the one named last changes fastest.
Arguments:
- one_query: float32 [7168, 7168], P('rows', 'width'), may hold values from -0.09375 to 0.09375
- other_query: float32 [7168, 7168], P('rows', 'width'), may hold values from -0.0625 to 0.0625
- one_key: float32 [7168, 1024], P('rows', 'width'), may hold values from -0.09375 to 0.09375
- other_key: float32 [7168, 1024], P('rows', 'width'), may hold values from -0.0625 to 0.0625
- one_value: float32 [7168, 1024], P('rows', 'width'), may hold values from -0.09375 to 0.09375
- other_value: float32 [7168, 1024], P('rows', 'width'), may hold values from -0.0625 to 0.0625
- mix_share: float32 [7168], P('rows'), may hold values from 0.2 to 0.8
- norm_train: float32 [7168], P(('rows', 'width')), may hold values from 0.25 to 1.75
- norm_step: float32 [7168], P(('rows', 'width')), may hold values from -0.3 to 0.3
Outputs:
- final_query: bfloat16 [7168, 7168], P(None, 'width')
- final_key: bfloat16 [7168, 1024], P(None, 'width')
- final_value: bfloat16 [7168, 1024], P(None, 'width')
- column_query: float32 [7168], P('width')
- column_key: float32 [1024], P('width')
- column_value: float32 [1024], P('width')
- serve_norm: bfloat16 [7168], replicated
The draws below stay inside these ranges and needn't reach their ends.
All inputs are finite; a program needn't handle non-finite values.
Results may differ from the reference program's by a relative error of at most 0.001.
Values may be sent and summed in bfloat16 or wider, within the bound.
A program may use at most 128 MiB of HBM per device.

```python
import jax
import jax.numpy as jnp
from jax import lax

D_MODEL = 7168
Q_DIM = 7168
KV_DIM = 1024


def spiked(result, rng, source, target, shards_of, factor):
    owner, partner = [(jnp.arange(result.shape[position]) // (result.shape[position] // shards_of)).reshape([-1 if axis == position else 1 for axis in range(result.ndim)]) for position in (source, target)]
    chosen = jax.random.permutation(rng, shards_of)[partner]
    strong = (owner == chosen) | (owner == (partner + shards_of // 2) % shards_of)
    return jnp.where(strong, factor * result, result)


def block_levels(stream_key, shape, shards, smallest, top_value):
    def one(position, shards_of):
        heights = jax.random.uniform(jax.random.fold_in(jax.random.fold_in(stream_key, 6), position), (shards_of,), jnp.float32, smallest / len(shards), top_value / len(shards))
        return jnp.repeat(jnp.exp(heights), shape[position] // shards_of).reshape((-1,) + (1,) * (len(shape) - position - 1))

    loudness = one(*shards[0])
    for cut in shards[1:]:
        loudness = loudness * one(*cut)
    return loudness


def bell_draw(rng, dims, deviation, most, cuts=(), dtype=jnp.bfloat16):
    entries = jax.random.normal(rng, dims, jnp.float32) * deviation
    if len(cuts) > 0:
        entries = block_levels(rng, dims, cuts, -0.22, 0.18) * entries
    return jnp.clip(entries, min=-most, max=most).astype(dtype)


def heavy_noise(key, extent, scale, most, split, heavy, dtype=jnp.bfloat16):
    values = scale * jax.random.normal(key, extent, jnp.float32)
    if split:
        values = values * block_levels(key, extent, split, -0.22, 0.18)
    return jnp.clip(spiked(values, jax.random.fold_in(key, 3), *heavy), -most, most).astype(dtype)


def setup_inputs(seed: int = 0) -> dict:
    seeds = jax.random.split(jax.random.key(seed), 10)
    return {
        "one_query": heavy_noise(seeds[0], (D_MODEL, Q_DIM), D_MODEL ** -0.5, 0.09375, ((0, 16), (1, 8)), (0, 1, 16, 2.0), jnp.float32),
        "other_query": bell_draw(seeds[1], (D_MODEL, Q_DIM), D_MODEL ** -0.5, 0.0625, ((0, 16), (1, 8)), jnp.float32),
        "one_key": heavy_noise(seeds[2], (D_MODEL, KV_DIM), D_MODEL ** -0.5, 0.09375, ((0, 16), (1, 8)), (0, 1, 16, 2.0), jnp.float32),
        "other_key": bell_draw(seeds[3], (D_MODEL, KV_DIM), D_MODEL ** -0.5, 0.0625, ((0, 16), (1, 8)), jnp.float32),
        "one_value": heavy_noise(seeds[4], (D_MODEL, KV_DIM), D_MODEL ** -0.5, 0.09375, ((0, 16), (1, 8)), (0, 1, 16, 2.0), jnp.float32),
        "other_value": bell_draw(seeds[5], (D_MODEL, KV_DIM), D_MODEL ** -0.5, 0.0625, ((0, 16), (1, 8)), jnp.float32),
        "mix_share": jnp.clip(0.2 + 0.6 * jax.random.uniform(seeds[6], (D_MODEL,), jnp.float32) ** block_levels(seeds[6], (D_MODEL,), ((0, 16),), -0.2, 0.2), 0.2, 0.8),
        "norm_train": jnp.clip(1.0 + 0.15 * jax.random.normal(seeds[7], (D_MODEL,), jnp.float32), 0.25, 1.75),
        "norm_step": jnp.clip(jax.random.uniform(seeds[8], (D_MODEL,), jnp.float32, -0.3, 0.3) * block_levels(seeds[8], (D_MODEL,), ((0, 128),), -0.4, 0.0), -0.3, 0.3),
    }


def reference(one_query, other_query, one_key, other_key, one_value, other_value, mix_share, norm_train, norm_step):
    result_query = mix_share[:, None] * one_query + (1.0 - mix_share[:, None]) * other_query
    result_key = mix_share[:, None] * one_key + (1.0 - mix_share[:, None]) * other_key
    result_value = mix_share[:, None] * one_value + (1.0 - mix_share[:, None]) * other_value
    column_query = jnp.sqrt(lax.optimization_barrier(jnp.sum(result_query * result_query, axis=0)))
    final_query = (result_query / column_query).astype(jnp.bfloat16)
    column_key = jnp.sqrt(lax.optimization_barrier(jnp.sum(result_key * result_key, axis=0)))
    final_key = (result_key / column_key).astype(jnp.bfloat16)
    column_value = jnp.sqrt(lax.optimization_barrier(jnp.sum(result_value * result_value, axis=0)))
    final_value = (result_value / column_value).astype(jnp.bfloat16)
    serve_norm = (norm_train + norm_step).astype(jnp.bfloat16)
    return (final_query, final_key, final_value, column_query, column_key, column_value, serve_norm)
```

```python
import jax
import jax.numpy as jnp
from jax import lax
from jax.experimental import pallas as pl
from jax.experimental.pallas import tpu as pltpu
from jax.sharding import PartitionSpec as P

MESH = pl.DeviceIdType.MESH
LANES = 128
DEVICES = 16
PEERS = 8
NORM = 56

PIECES = ((0, 96), (96, 96), (192, 128), (320, 128))
LOADS = 4


def gather_kernel(
    one_query,
    other_query,
    one_key,
    other_key,
    one_value,
    other_value,
    mix,
    train,
    step,
    blocks,
    scale_query,
    scale_key,
    scale_value,
    serve,
    ones,
    others,
    mixed,
    shares,
    share_row,
    mix_here,
    train_here,
    step_here,
    sums,
    norm_row,
    norm_images,
    norm_pairs,
    norm_all,
    load_sem,
    small_sem,
    send_sem,
    recv_sem,
    sum_send,
    sum_recv,
    image_send,
    image_recv,
    pair_send,
    pair_recv,
):
    depth = mixed.shape[0]
    me = lax.axis_index("rows")
    place = lax.axis_index("width")
    core = lax.rem(me, 2)
    y = lax.rem(lax.div(me, 2), 4)
    z = lax.div(me, 8)

    def device(dz, dy, other=0):
        return lax.rem(z + dz, 2) * 8 + lax.rem(y + dy, 4) * 2 + lax.rem(core + other, 2)

    up, down, across, sibling = device(0, 1), device(0, 3), device(1, 0), device(0, 0, 1)

    small = []
    for i, (source, target) in enumerate(
        ((mix, mix_here), (train, train_here), (step, step_here))
    ):
        copy = pltpu.make_async_copy(source, target, small_sem.at[i])
        copy.start()
        small.append(copy)
    pairs = ((one_query, other_query), (one_key, other_key), (one_value, other_value))
    chunk = depth // LOADS
    loads = []
    for i in range(LOADS):
        mine = []
        at = 0
        for a, (one, other) in enumerate(pairs):
            wide = one.shape[1]
            for b, (source, target) in enumerate(((one, ones), (other, others))):
                rows = pl.ds(i * chunk, chunk)
                copy = pltpu.make_async_copy(
                    source.at[rows, :], target.at[rows, pl.ds(at, wide)], load_sem.at[i, 2 * a + b]
                )
                copy.start()
                mine.append(copy)
            at += wide
        loads.append(mine)

    barrier = pltpu.get_barrier_semaphore()
    for j in range(1, DEVICES):
        pl.semaphore_signal(
            barrier, inc=1, device_id={"rows": lax.rem(me + j, DEVICES)}, device_id_type=MESH
        )
    for j in range(1, PEERS):
        pl.semaphore_signal(
            barrier, inc=1, device_id={"width": lax.rem(place + j, PEERS)}, device_id_type=MESH
        )

    for copy in small:
        copy.wait()

    share_row[...] = jnp.zeros_like(share_row)
    share_row[:, pl.ds(0, depth)] = mix_here[...]
    for i in range(shares.shape[0] // LANES):
        row = share_row[:, pl.ds(i * LANES, LANES)]
        shares[pl.ds(i * LANES, LANES), :] = jnp.broadcast_to(row, (LANES, LANES)).T

    norm_row[...] = jnp.zeros_like(norm_row)
    norm_row[:, pl.ds(0, NORM)] = train_here[...] + step_here[...]
    first = (lax.rem(me, 2) * PEERS + place) * NORM
    gains = jnp.broadcast_to(norm_row[...], (8, LANES))
    gains = pltpu.roll(gains, lax.rem(first, LANES), 1)
    flat = lax.broadcasted_iota(jnp.int32, (8, LANES), 0) * LANES + lax.broadcasted_iota(
        jnp.int32, (8, LANES), 1
    )
    inside = (flat >= first) & (flat < first + NORM)
    norm_images[place] = jnp.where(inside, gains, 0.0)

    tiles = mixed.shape[1] // LANES

    def mix_rows(strip, partial):
        rows = pl.ds(pl.multiple_of(strip * 8, 8), 8)
        share = shares[rows, :]
        rest = 1.0 - share
        found = []
        for t in range(tiles):
            lanes = pl.ds(t * LANES, LANES)
            value = share * ones[rows, lanes] + rest * others[rows, lanes]
            mixed[rows, lanes] = value
            found.append(partial[t] + value * value)
        return tuple(found)

    partial = tuple(jnp.zeros((8, LANES), jnp.float32) for _ in range(tiles))
    for i in range(LOADS):
        for copy in loads[i]:
            copy.wait()
        partial = lax.fori_loop(i * chunk // 8, (i + 1) * chunk // 8, mix_rows, partial, unroll=2)
    for t in range(tiles):
        sums[me, :, pl.ds(t * LANES, LANES)] = jnp.sum(partial[t], axis=0, keepdims=True)

    pl.semaphore_wait(barrier, DEVICES - 1 + PEERS - 1)

    sum_copies = []
    for j in range(1, DEVICES):
        copy = pltpu.make_async_remote_copy(
            src_ref=sums.at[me],
            dst_ref=sums.at[me],
            send_sem=sum_send.at[j],
            recv_sem=sum_recv.at[me],
            device_id={"rows": lax.rem(me + j, DEVICES)},
            device_id_type=MESH,
        )
        copy.start()
        sum_copies.append(copy)
    image_copies = []
    for j in range(1, PEERS):
        copy = pltpu.make_async_remote_copy(
            src_ref=norm_images.at[place],
            dst_ref=norm_images.at[place],
            send_sem=image_send.at[j],
            recv_sem=image_recv.at[place],
            device_id={"width": lax.rem(place + j, PEERS)},
            device_id_type=MESH,
        )
        copy.start()
        image_copies.append(copy)

    for j in range(1, DEVICES):
        source = lax.rem(me + j, DEVICES)
        pltpu.make_async_remote_copy(
            src_ref=sums.at[source],
            dst_ref=sums.at[source],
            send_sem=sum_send.at[j],
            recv_sem=sum_recv.at[source],
            device_id={"rows": source},
            device_id_type=MESH,
        ).wait_recv()

    total = sums[0]
    for j in range(1, DEVICES):
        total = total + sums[j]
    scale = jnp.sqrt(total)
    t = 0
    for out in (scale_query, scale_key, scale_value):
        for i in range(out.shape[0]):
            out[i : i + 1, :] = scale[:, t * LANES : (t + 1) * LANES]
            t += 1
    inverse = 1.0 / scale
    factors = [
        jnp.broadcast_to(inverse[:, t * LANES : (t + 1) * LANES], (16, LANES)) for t in range(tiles)
    ]

    def narrow(piece):
        start, count = PIECES[piece]

        def body(strip, carry):
            rows = pl.ds(pl.multiple_of(start + strip * 16, 16), 16)
            for t in range(tiles):
                lanes = pl.ds(t * LANES, LANES)
                blocks[me, rows, lanes] = (mixed[rows, lanes] * factors[t]).astype(jnp.bfloat16)
            return carry

        lax.fori_loop(0, count // 16, body, 0, unroll=2)

    sent = []

    def send(block, piece, target):
        rows = pl.ds(*PIECES[piece])
        copy = pltpu.make_async_remote_copy(
            src_ref=blocks.at[block, rows, :],
            dst_ref=blocks.at[block, rows, :],
            send_sem=send_sem.at[len(sent)],
            recv_sem=recv_sem.at[block, piece],
            device_id={"rows": target},
            device_id_type=MESH,
        )
        copy.start()
        sent.append(copy)

    def arrived(block, piece):
        rows = pl.ds(*PIECES[piece])
        pltpu.make_async_remote_copy(
            src_ref=blocks.at[block, rows, :],
            dst_ref=blocks.at[block, rows, :],
            send_sem=send_sem.at[0],
            recv_sem=recv_sem.at[block, piece],
            device_id={"rows": sibling},
            device_id_type=MESH,
        ).wait_recv()

    narrow(0)
    send(me, 0, up)
    narrow(1)
    send(me, 1, down)
    send(me, 1, up)
    send(me, 0, down)
    narrow(2)
    send(me, 2, across)
    send(me, 2, up)
    narrow(3)
    send(me, 3, down)
    send(me, 3, across)
    send(me, 3, up)
    send(me, 2, down)
    send(me, 0, across)
    send(me, 1, across)
    for piece in range(4):
        send(me, piece, sibling)

    for j in range(1, PEERS):
        source = lax.rem(place + j, PEERS)
        pltpu.make_async_remote_copy(
            src_ref=norm_images.at[source],
            dst_ref=norm_images.at[source],
            send_sem=image_send.at[j],
            recv_sem=image_recv.at[source],
            device_id={"width": source},
            device_id_type=MESH,
        ).wait_recv()
    image = norm_images[0]
    for j in range(1, PEERS):
        image = image + norm_images[j]
    norm_pairs[me] = image
    pair_copies = []
    for j in range(1, DEVICES):
        copy = pltpu.make_async_remote_copy(
            src_ref=norm_pairs.at[me],
            dst_ref=norm_pairs.at[me],
            send_sem=pair_send.at[j],
            recv_sem=pair_recv.at[me],
            device_id={"rows": lax.rem(me + j, DEVICES)},
            device_id_type=MESH,
        )
        copy.start()
        pair_copies.append(copy)

    below, above, far = device(0, 3), device(0, 1), device(0, 2)
    side, side_below, side_above, side_far = device(1, 0), device(1, 3), device(1, 1), device(1, 2)
    seen = set()
    for block, piece, targets in (
        (below, 0, (up, across)),
        (above, 1, (down, across)),
        (side, 2, (up,)),
        (below, 1, (across,)),
        (above, 0, (across,)),
        (side, 3, (down, up)),
        (side, 2, (down,)),
        (below, 2, (up,)),
        (above, 3, (down,)),
        (side, 0, ()),
        (below, 3, ()),
        (above, 2, ()),
        (side, 1, ()),
        (far, 0, (across,)),
        (far, 1, (across,)),
        (side_below, 0, ()),
        (side_above, 1, ()),
        (side_below, 2, (up,)),
        (side_above, 3, (down,)),
        (side_below, 1, ()),
        (side_below, 3, ()),
        (side_above, 2, ()),
        (side_above, 0, ()),
        (far, 2, ()),
        (far, 3, ()),
        (side_far, 0, ()),
        (side_far, 1, ()),
        (side_far, 2, ()),
        (side_far, 3, ()),
    ):
        if (id(block), piece) not in seen:
            seen.add((id(block), piece))
            arrived(block, piece)
            send(block, piece, sibling)
        for target in targets:
            send(block, piece, target)

    for j in range(1, DEVICES):
        source = lax.rem(me + j, DEVICES)
        pltpu.make_async_remote_copy(
            src_ref=norm_pairs.at[source],
            dst_ref=norm_pairs.at[source],
            send_sem=pair_send.at[j],
            recv_sem=pair_recv.at[source],
            device_id={"rows": source},
            device_id_type=MESH,
        ).wait_recv()
    for j in range(DEVICES // 2):
        both = norm_pairs[2 * j] + norm_pairs[2 * j + 1]
        norm_all[pl.ds(7 * j, 8), :] = both
    serve[...] = norm_all[pl.ds(0, NORM), :].astype(serve.dtype)

    for dz in range(2):
        for dy in range(4):
            for piece in range(4):
                arrived(device(dz, dy, 1), piece)
    for copy in sent + sum_copies + image_copies + pair_copies:
        copy.wait_send()


def write_kernel(
    blocks,
    scale_query,
    scale_key,
    scale_value,
    serve,
    query,
    key,
    value,
    query_scale,
    key_scale,
    value_scale,
    gains,
    sem,
    small_sem,
):
    depth = blocks.shape[1]
    copies = []
    for b in range(DEVICES):
        at = 0
        for n, out in enumerate((query, key, value)):
            wide = out.shape[1]
            copy = pltpu.make_async_copy(
                blocks.at[b, :, pl.ds(at, wide)], out.at[pl.ds(b * depth, depth), :], sem.at[b, n]
            )
            copy.start()
            copies.append(copy)
            at += wide
    for i, (source, target) in enumerate(
        (
            (scale_query, query_scale),
            (scale_key, key_scale),
            (scale_value, value_scale),
            (serve, gains),
        )
    ):
        copy = pltpu.make_async_copy(source, target, small_sem.at[i])
        copy.start()
        copies.append(copy)
    for copy in copies:
        copy.wait()


def shards(
    one_query,
    other_query,
    one_key,
    other_key,
    one_value,
    other_value,
    mix_share,
    norm_train,
    norm_step,
):
    f32, bf16 = jnp.float32, jnp.bfloat16
    depth, queries = one_query.shape
    keys = one_key.shape[1]
    wide = queries + 2 * keys
    tall = -(-depth // LANES) * LANES
    dma = pltpu.SemaphoreType.DMA
    hbm, vmem = pl.BlockSpec(memory_space=pltpu.HBM), pl.BlockSpec(memory_space=pltpu.VMEM)
    blocks, scale_query, scale_key, scale_value, serve = pl.pallas_call(
        gather_kernel,
        out_shape=(
            pltpu.VMEM((DEVICES, depth, wide), bf16),
            pltpu.VMEM((queries // LANES, LANES), f32),
            pltpu.VMEM((keys // LANES, LANES), f32),
            pltpu.VMEM((keys // LANES, LANES), f32),
            pltpu.VMEM((NORM, LANES), bf16),
        ),
        in_specs=[hbm] * 9,
        out_specs=[vmem] * 5,
        scratch_shapes=[
            pltpu.VMEM((depth, wide), f32),
            pltpu.VMEM((depth, wide), f32),
            pltpu.VMEM((depth, wide), f32),
            pltpu.VMEM((tall, LANES), f32),
            pltpu.VMEM((1, tall), f32),
            pltpu.VMEM((1, depth), f32),
            pltpu.VMEM((1, NORM), f32),
            pltpu.VMEM((1, NORM), f32),
            pltpu.VMEM((DEVICES, 1, wide), f32),
            pltpu.VMEM((1, LANES), f32),
            pltpu.VMEM((PEERS, 8, LANES), f32),
            pltpu.VMEM((DEVICES, 8, LANES), f32),
            pltpu.VMEM((64, LANES), f32),
            dma((LOADS, 6)),
            dma((3,)),
            dma((72,)),
            dma((DEVICES, 4)),
            dma((DEVICES,)),
            dma((DEVICES,)),
            dma((PEERS,)),
            dma((PEERS,)),
            dma((DEVICES,)),
            dma((DEVICES,)),
        ],
        compiler_params=pltpu.CompilerParams(
            collective_id=0, has_side_effects=True, vmem_limit_bytes=48 * 1024 * 1024
        ),
        name="gather",
    )(
        one_query,
        other_query,
        one_key,
        other_key,
        one_value,
        other_value,
        mix_share.reshape(1, depth),
        norm_train.reshape(1, NORM),
        norm_step.reshape(1, NORM),
    )
    finals = pl.pallas_call(
        write_kernel,
        out_shape=(
            jax.ShapeDtypeStruct((DEVICES * depth, queries), bf16),
            jax.ShapeDtypeStruct((DEVICES * depth, keys), bf16),
            jax.ShapeDtypeStruct((DEVICES * depth, keys), bf16),
            jax.ShapeDtypeStruct((queries // LANES, LANES), f32),
            jax.ShapeDtypeStruct((keys // LANES, LANES), f32),
            jax.ShapeDtypeStruct((keys // LANES, LANES), f32),
            jax.ShapeDtypeStruct((NORM, LANES), bf16),
        ),
        in_specs=[vmem] * 5,
        out_specs=[hbm] * 7,
        scratch_shapes=[dma((DEVICES, 3)), dma((4,))],
        compiler_params=pltpu.CompilerParams(vmem_limit_bytes=1024 * 1024),
        name="write",
    )(blocks, scale_query, scale_key, scale_value, serve)
    return finals[:3] + tuple(a.reshape(-1) for a in finals[3:])


def solution(mesh):
    in_specs = (
        P("rows", "width"),
        P("rows", "width"),
        P("rows", "width"),
        P("rows", "width"),
        P("rows", "width"),
        P("rows", "width"),
        P("rows"),
        P(("rows", "width")),
        P(("rows", "width")),
    )
    out_specs = (
        P(None, "width"),
        P(None, "width"),
        P(None, "width"),
        P("width"),
        P("width"),
        P("width"),
        P(),
    )
    return jax.shard_map(shards, mesh=mesh, in_specs=in_specs, out_specs=out_specs, check_vma=False)
```

```python
import jax
import jax.numpy as jnp
from jax import lax
from jax.experimental import pallas as pl
from jax.experimental.pallas import tpu as pltpu
from jax.sharding import PartitionSpec as P

MESH = pl.DeviceIdType.MESH
LANES = 128
DEVICES = 16
PEERS = 8
NORM = 56

PIECES = ((0, 96), (96, 96), (192, 128), (320, 128))
LOADS = 4


def gather_kernel(
    one_query,
    other_query,
    one_key,
    other_key,
    one_value,
    other_value,
    mix,
    train,
    step,
    blocks,
    scale_query,
    scale_key,
    scale_value,
    serve,
    both,
    mixed,
    shares,
    share_row,
    mix_here,
    train_here,
    step_here,
    sums,
    norm_row,
    norm_images,
    norm_pairs,
    norm_all,
    load_sem,
    small_sem,
    send_sem,
    recv_sem,
    sibling_sem,
    sum_sem,
    image_send,
    image_recv,
    pair_sem,
):
    depth, wide = mixed.shape
    tiles = wide // LANES
    me = lax.axis_index("rows")
    place = lax.axis_index("width")
    core = lax.rem(me, 2)
    y = lax.rem(lax.div(me, 2), 4)
    z = lax.div(me, 8)

    def device(dz, dy, other=0):
        return lax.rem(z + dz, 2) * 8 + lax.rem(y + dy, 4) * 2 + lax.rem(core + other, 2)

    def remote(ref, send, recv, **target):
        return pltpu.make_async_remote_copy(
            src_ref=ref,
            dst_ref=ref,
            send_sem=send,
            recv_sem=recv,
            device_id=target,
            device_id_type=MESH,
        )

    def wait_bytes(ref, sem):
        pltpu.make_async_copy(ref, ref, sem).wait()

    for i, (source, target) in enumerate(
        ((mix, mix_here), (train, train_here), (step, step_here))
    ):
        pltpu.make_async_copy(source, target, small_sem.at[i]).start()
    chunk = depth // LOADS
    for i in range(LOADS):
        rows = pl.ds(i * chunk, chunk)
        at = 0
        for pair in ((one_query, other_query), (one_key, other_key), (one_value, other_value)):
            for n, source in enumerate(pair):
                columns = pl.ds(at, source.shape[1])
                pltpu.make_async_copy(
                    source.at[rows, :], both.at[n, rows, columns], load_sem.at[i]
                ).start()
            at += pair[0].shape[1]

    barrier = pltpu.get_barrier_semaphore()
    for j in range(1, DEVICES):
        pl.semaphore_signal(
            barrier, inc=1, device_id={"rows": lax.rem(me + j, DEVICES)}, device_id_type=MESH
        )
    for j in range(1, PEERS):

        @pl.when(place + j < PEERS)
        def _():
            pl.semaphore_signal(
                barrier, inc=1, device_id={"width": place + j}, device_id_type=MESH
            )

    for i, target in enumerate((mix_here, train_here, step_here)):
        wait_bytes(target, small_sem.at[i])

    share_row[...] = jnp.zeros_like(share_row)
    share_row[:, pl.ds(0, depth)] = mix_here[...]
    for i in range(shares.shape[0] // LANES):
        row = share_row[:, pl.ds(i * LANES, LANES)]
        shares[pl.ds(i * LANES, LANES), :] = jnp.broadcast_to(row, (LANES, LANES)).T

    norm_row[...] = jnp.zeros_like(norm_row)
    norm_row[:, pl.ds(0, NORM)] = train_here[...] + step_here[...]
    first = (core * PEERS + place) * NORM
    gains = jnp.broadcast_to(norm_row[...], (8, LANES))
    gains = pltpu.roll(gains, lax.rem(first, LANES), 1)
    flat = lax.broadcasted_iota(jnp.int32, (8, LANES), 0) * LANES + lax.broadcasted_iota(
        jnp.int32, (8, LANES), 1
    )
    inside = (flat >= first) & (flat < first + NORM)
    norm_images[place] = jnp.where(inside, gains, 0.0)

    def mix_rows(strip, partial):
        rows = pl.ds(pl.multiple_of(strip * 8, 8), 8)
        share = shares[rows, :]
        rest = 1.0 - share
        found = []
        for t in range(tiles):
            lanes = pl.ds(t * LANES, LANES)
            value = share * both[0, rows, lanes] + rest * both[1, rows, lanes]
            mixed[rows, lanes] = value
            found.append(partial[t] + value * value)
        return tuple(found)

    partial = tuple(jnp.zeros((8, LANES), jnp.float32) for _ in range(tiles))
    for i in range(LOADS):
        wait_bytes(both.at[:, pl.ds(i * chunk, chunk), :], load_sem.at[i])
        partial = lax.fori_loop(i * chunk // 8, (i + 1) * chunk // 8, mix_rows, partial, unroll=2)
    for t in range(tiles):
        sums[me, :, pl.ds(t * LANES, LANES)] = jnp.sum(partial[t], axis=0, keepdims=True)

    pl.semaphore_wait(barrier, DEVICES - 1 + place)

    for j in range(1, DEVICES):
        remote(sums.at[me], sum_sem.at[0], sum_sem.at[1], rows=lax.rem(me + j, DEVICES)).start()

    def image_copy(source, target):
        return remote(norm_images.at[source], image_send.at[0], image_recv.at[source], width=target)

    for j in range(1, PEERS):

        @pl.when(place + j >= PEERS)
        def _():
            image_copy(place, place + j - PEERS).start()

    wait_bytes(sums.at[pl.ds(0, DEVICES - 1)], sum_sem.at[1])
    total = sums[0]
    for j in range(1, DEVICES):
        total = total + sums[j]
    scale = jnp.sqrt(total)
    t = 0
    for out in (scale_query, scale_key, scale_value):
        for i in range(out.shape[0]):
            out[i : i + 1, :] = scale[:, t * LANES : (t + 1) * LANES]
            t += 1
    inverse = 1.0 / scale
    factors = [
        jnp.broadcast_to(inverse[:, t * LANES : (t + 1) * LANES], (16, LANES)) for t in range(tiles)
    ]

    def narrow(piece):
        start, count = PIECES[piece]

        def body(strip, carry):
            rows = pl.ds(pl.multiple_of(start + strip * 16, 16), 16)
            for t in range(tiles):
                lanes = pl.ds(t * LANES, LANES)
                blocks[me, rows, lanes] = (mixed[rows, lanes] * factors[t]).astype(jnp.bfloat16)
            return carry

        lax.fori_loop(0, count // 16, body, 0, unroll=2)

    up, down, across, sibling = (0, 1), (0, 3), (1, 0), None
    rows_sent = [0]

    def piece_copy(block, piece, target):
        rows = pl.ds(*PIECES[piece])
        if target is sibling:
            recv = sibling_sem.at[0]
            goal = device(0, 0, 1)
        else:
            recv = recv_sem.at[(block[0] - target[0]) % 2 * 4 + (block[1] - target[1]) % 4, piece]
            goal = device(*target)
        return remote(blocks.at[device(*block), rows, :], send_sem.at[0], recv, rows=goal)

    def send(block, piece, target):
        piece_copy(block, piece, target).start()
        rows_sent[0] += PIECES[piece][1]

    def arrived(block, piece):
        wait_bytes(
            blocks.at[device(*block), pl.ds(*PIECES[piece]), :],
            recv_sem.at[block[0] * 4 + block[1], piece],
        )

    own = (0, 0)
    narrow(0)
    send(own, 0, up)
    narrow(1)
    send(own, 1, down)
    send(own, 1, up)
    send(own, 0, down)
    narrow(2)
    send(own, 2, across)
    send(own, 2, up)
    narrow(3)
    send(own, 3, down)
    send(own, 3, across)
    send(own, 3, up)
    send(own, 2, down)
    send(own, 0, across)
    send(own, 1, across)
    for piece in range(4):
        send(own, piece, sibling)

    below, above, far = (0, 3), (0, 1), (0, 2)
    side, side_below, side_above, side_far = (1, 0), (1, 3), (1, 1), (1, 2)
    for block, piece, targets in (
        (below, 0, (up, across)),
        (above, 1, (down, across)),
        (side, 2, (up,)),
        (below, 1, (across,)),
        (above, 0, (across,)),
        (side, 3, (down, up)),
        (side, None, ()),
        (below, 2, (up,)),
        (above, 3, (down,)),
        (side, 0, ()),
        (below, 3, ()),
        (above, 2, ()),
        (side, 1, ()),
    ):
        if piece is None:
            send(side, 2, down)
            continue
        arrived(block, piece)
        for target in targets + (sibling,):
            send(block, piece, target)

    for j in range(1, PEERS):

        @pl.when(place + j < PEERS)
        def _():
            image_copy(place + j, place).wait_recv()
            image_copy(place, place + j).start()

    for block, piece, targets in (
        (far, 0, (across,)),
        (far, 1, (across,)),
        (side_below, 0, ()),
        (side_above, 1, ()),
        (side_below, 2, (up,)),
        (side_above, 3, (down,)),
        (side_below, 1, ()),
    ):
        arrived(block, piece)
        for target in targets + (sibling,):
            send(block, piece, target)

    for j in range(1, PEERS):

        @pl.when(place + j >= PEERS)
        def _():
            image_copy(place + j - PEERS, place).wait_recv()

    image = norm_images[0]
    for j in range(1, PEERS):
        image = image + norm_images[j]
    norm_pairs[me] = image
    for j in range(1, DEVICES):
        remote(
            norm_pairs.at[me], pair_sem.at[0], pair_sem.at[1], rows=lax.rem(me + j, DEVICES)
        ).start()

    for block, piece in (
        (side_below, 3),
        (side_above, 2),
        (side_above, 0),
        (far, 2),
        (far, 3),
        (side_far, 0),
    ):
        arrived(block, piece)
        send(block, piece, sibling)

    wait_bytes(norm_pairs.at[pl.ds(0, DEVICES - 1)], pair_sem.at[1])
    for j in range(DEVICES // 2):
        norm_all[pl.ds(7 * j, 8), :] = norm_pairs[2 * j] + norm_pairs[2 * j + 1]
    serve[...] = norm_all[pl.ds(0, NORM), :].astype(serve.dtype)
    wait_bytes(sums.at[pl.ds(0, DEVICES - 1)], sum_sem.at[0])
    wait_bytes(norm_images.at[pl.ds(0, PEERS - 1)], image_send.at[0])
    wait_bytes(norm_pairs.at[pl.ds(0, DEVICES - 1)], pair_sem.at[0])

    for block, piece in ((side_far, 1), (side_far, 2), (side_far, 3)):
        arrived(block, piece)
        send(block, piece, sibling)

    wait_bytes(blocks.at[pl.ds(0, DEVICES // 2)], sibling_sem.at[0])
    assert rows_sent[0] % depth == 0
    wait_bytes(blocks.at[pl.ds(0, rows_sent[0] // depth)], send_sem.at[0])


def write_kernel(
    blocks,
    scale_query,
    scale_key,
    scale_value,
    serve,
    query,
    key,
    value,
    query_scale,
    key_scale,
    value_scale,
    gains,
    sem,
    small_sem,
):
    depth = blocks.shape[1]
    outs = (query, key, value)
    for b in range(DEVICES):
        at = 0
        for n, out in enumerate(outs):
            pltpu.make_async_copy(
                blocks.at[b, :, pl.ds(at, out.shape[1])],
                out.at[pl.ds(b * depth, depth), :],
                sem.at[n],
            ).start()
            at += out.shape[1]
    small = (
        (scale_query, query_scale),
        (scale_key, key_scale),
        (scale_value, value_scale),
        (serve, gains),
    )
    for i, (source, target) in enumerate(small):
        pltpu.make_async_copy(source, target, small_sem.at[i]).start()
    for n, out in enumerate(outs):
        pltpu.make_async_copy(out, out, sem.at[n]).wait()
    for i, (source, target) in enumerate(small):
        pltpu.make_async_copy(source, target, small_sem.at[i]).wait()


def shards(
    one_query,
    other_query,
    one_key,
    other_key,
    one_value,
    other_value,
    mix_share,
    norm_train,
    norm_step,
):
    f32, bf16 = jnp.float32, jnp.bfloat16
    depth, queries = one_query.shape
    keys = one_key.shape[1]
    wide = queries + 2 * keys
    tall = -(-depth // LANES) * LANES
    dma = pltpu.SemaphoreType.DMA
    hbm, vmem = pl.BlockSpec(memory_space=pltpu.HBM), pl.BlockSpec(memory_space=pltpu.VMEM)
    blocks, scale_query, scale_key, scale_value, serve = pl.pallas_call(
        gather_kernel,
        out_shape=(
            pltpu.VMEM((DEVICES, depth, wide), bf16),
            pltpu.VMEM((queries // LANES, LANES), f32),
            pltpu.VMEM((keys // LANES, LANES), f32),
            pltpu.VMEM((keys // LANES, LANES), f32),
            pltpu.VMEM((NORM, LANES), bf16),
        ),
        in_specs=[hbm] * 9,
        out_specs=[vmem] * 5,
        scratch_shapes=[
            pltpu.VMEM((2, depth, wide), f32),
            pltpu.VMEM((depth, wide), f32),
            pltpu.VMEM((tall, LANES), f32),
            pltpu.VMEM((1, tall), f32),
            pltpu.VMEM((1, depth), f32),
            pltpu.VMEM((1, NORM), f32),
            pltpu.VMEM((1, NORM), f32),
            pltpu.VMEM((DEVICES, 1, wide), f32),
            pltpu.VMEM((1, LANES), f32),
            pltpu.VMEM((PEERS, 8, LANES), f32),
            pltpu.VMEM((DEVICES, 8, LANES), f32),
            pltpu.VMEM((64, LANES), f32),
            dma((LOADS,)),
            dma((3,)),
            dma((1,)),
            dma((8, 4)),
            dma((1,)),
            dma((2,)),
            dma((1,)),
            dma((PEERS,)),
            dma((2,)),
        ],
        compiler_params=pltpu.CompilerParams(
            collective_id=0, has_side_effects=True, vmem_limit_bytes=48 * 1024 * 1024
        ),
        name="gather",
    )(
        one_query,
        other_query,
        one_key,
        other_key,
        one_value,
        other_value,
        mix_share.reshape(1, depth),
        norm_train.reshape(1, NORM),
        norm_step.reshape(1, NORM),
    )
    finals = pl.pallas_call(
        write_kernel,
        out_shape=(
            jax.ShapeDtypeStruct((DEVICES * depth, queries), bf16),
            jax.ShapeDtypeStruct((DEVICES * depth, keys), bf16),
            jax.ShapeDtypeStruct((DEVICES * depth, keys), bf16),
            jax.ShapeDtypeStruct((queries // LANES, LANES), f32),
            jax.ShapeDtypeStruct((keys // LANES, LANES), f32),
            jax.ShapeDtypeStruct((keys // LANES, LANES), f32),
            jax.ShapeDtypeStruct((NORM, LANES), bf16),
        ),
        in_specs=[vmem] * 5,
        out_specs=[hbm] * 7,
        scratch_shapes=[dma((3,)), dma((4,))],
        compiler_params=pltpu.CompilerParams(vmem_limit_bytes=1024 * 1024),
        name="write",
    )(blocks, scale_query, scale_key, scale_value, serve)
    return finals[:3] + tuple(a.reshape(-1) for a in finals[3:])


def solution(mesh):
    in_specs = (
        P("rows", "width"),
        P("rows", "width"),
        P("rows", "width"),
        P("rows", "width"),
        P("rows", "width"),
        P("rows", "width"),
        P("rows"),
        P(("rows", "width")),
        P(("rows", "width")),
    )
    out_specs = (
        P(None, "width"),
        P(None, "width"),
        P(None, "width"),
        P("width"),
        P("width"),
        P("width"),
        P(),
    )
    return jax.shard_map(shards, mesh=mesh, in_specs=in_specs, out_specs=out_specs, check_vma=False)
```

```python
import jax
import jax.numpy as jnp
from jax import lax
from jax.experimental import pallas as pl
from jax.experimental.pallas import tpu as pltpu
from jax.sharding import PartitionSpec as P

MESH = pl.DeviceIdType.MESH
LANES = 128
DEVICES = 16
PEERS = 8
NORM = 56

PIECES = ((0, 96), (96, 96), (192, 128), (320, 128))
LOADS = 4


def gather_kernel(
    one_query,
    other_query,
    one_key,
    other_key,
    one_value,
    other_value,
    mix,
    train,
    step,
    blocks,
    scale_query,
    scale_key,
    scale_value,
    serve,
    both,
    mixed,
    shares,
    share_row,
    mix_here,
    train_here,
    step_here,
    sums,
    norm_row,
    norm_images,
    norm_pairs,
    norm_all,
    load_sem,
    small_sem,
    send_sem,
    recv_sem,
    sibling_sem,
    sum_sem,
    image_send,
    image_recv,
    pair_sem,
):
    depth, wide = mixed.shape
    tiles = wide // LANES
    me = lax.axis_index("rows")
    place = lax.axis_index("width")
    core = lax.rem(me, 2)
    y = lax.rem(lax.div(me, 2), 4)
    z = lax.div(me, 8)

    def device(dz, dy, other=0):
        return lax.rem(z + dz, 2) * 8 + lax.rem(y + dy, 4) * 2 + lax.rem(core + other, 2)

    def remote(ref, send, recv, **target):
        return pltpu.make_async_remote_copy(
            src_ref=ref,
            dst_ref=ref,
            send_sem=send,
            recv_sem=recv,
            device_id=target,
            device_id_type=MESH,
        )

    def wait_bytes(ref, sem):
        pltpu.make_async_copy(ref, ref, sem).wait()

    for i, (source, target) in enumerate(
        ((mix, mix_here), (train, train_here), (step, step_here))
    ):
        pltpu.make_async_copy(source, target, small_sem.at[i]).start()
    chunk = depth // LOADS
    for i in range(LOADS):
        rows = pl.ds(i * chunk, chunk)
        at = 0
        for pair in ((one_query, other_query), (one_key, other_key), (one_value, other_value)):
            for n, source in enumerate(pair):
                columns = pl.ds(at, source.shape[1])
                pltpu.make_async_copy(
                    source.at[rows, :], both.at[n, rows, columns], load_sem.at[i]
                ).start()
            at += pair[0].shape[1]

    barrier = pltpu.get_barrier_semaphore()
    for j in range(1, DEVICES):
        pl.semaphore_signal(
            barrier, inc=1, device_id={"rows": lax.rem(me + j, DEVICES)}, device_id_type=MESH
        )
    for j in range(1, PEERS):

        @pl.when(place + j < PEERS)
        def _():
            pl.semaphore_signal(
                barrier, inc=1, device_id={"width": place + j}, device_id_type=MESH
            )

    for i, target in enumerate((mix_here, train_here, step_here)):
        wait_bytes(target, small_sem.at[i])

    share_row[...] = jnp.zeros_like(share_row)
    share_row[:, pl.ds(0, depth)] = mix_here[...]
    for i in range(shares.shape[0] // LANES):
        row = share_row[:, pl.ds(i * LANES, LANES)]
        shares[pl.ds(i * LANES, LANES), :] = jnp.broadcast_to(row, (LANES, LANES)).T

    norm_row[...] = jnp.zeros_like(norm_row)
    norm_row[:, pl.ds(0, NORM)] = train_here[...] + step_here[...]
    first = (core * PEERS + place) * NORM
    gains = jnp.broadcast_to(norm_row[...], (8, LANES))
    gains = pltpu.roll(gains, lax.rem(first, LANES), 1)
    flat = lax.broadcasted_iota(jnp.int32, (8, LANES), 0) * LANES + lax.broadcasted_iota(
        jnp.int32, (8, LANES), 1
    )
    inside = (flat >= first) & (flat < first + NORM)
    norm_images[place] = jnp.where(inside, gains, 0.0)

    def mix_rows(strip, partial):
        rows = pl.ds(pl.multiple_of(strip * 8, 8), 8)
        share = shares[rows, :]
        rest = 1.0 - share
        found = []
        for t in range(tiles):
            lanes = pl.ds(t * LANES, LANES)
            value = share * both[0, rows, lanes] + rest * both[1, rows, lanes]
            mixed[rows, lanes] = value
            found.append(partial[t] + value * value)
        return tuple(found)

    partial = tuple(jnp.zeros((8, LANES), jnp.float32) for _ in range(tiles))
    for i in range(LOADS):
        wait_bytes(both.at[:, pl.ds(i * chunk, chunk), :], load_sem.at[i])
        partial = lax.fori_loop(i * chunk // 8, (i + 1) * chunk // 8, mix_rows, partial, unroll=2)
    for t in range(tiles):
        sums[me, :, pl.ds(t * LANES, LANES)] = jnp.sum(partial[t], axis=0, keepdims=True)

    pl.semaphore_wait(barrier, DEVICES - 1 + place)

    for j in range(1, DEVICES):
        remote(sums.at[me], sum_sem.at[0], sum_sem.at[1], rows=lax.rem(me + j, DEVICES)).start()

    def image_copy(source, target):
        return remote(norm_images.at[source], image_send.at[0], image_recv.at[source], width=target)

    for j in range(1, PEERS):

        @pl.when(place + j >= PEERS)
        def _():
            image_copy(place, place + j - PEERS).start()

    wait_bytes(sums.at[pl.ds(0, DEVICES - 1)], sum_sem.at[1])
    total = sums[0]
    for j in range(1, DEVICES):
        total = total + sums[j]
    scale = jnp.sqrt(total)
    t = 0
    for out in (scale_query, scale_key, scale_value):
        for i in range(out.shape[0]):
            out[i : i + 1, :] = scale[:, t * LANES : (t + 1) * LANES]
            t += 1
    inverse = 1.0 / scale
    factors = [
        jnp.broadcast_to(inverse[:, t * LANES : (t + 1) * LANES], (16, LANES)) for t in range(tiles)
    ]

    def narrow(piece):
        start, count = PIECES[piece]

        def body(strip, carry):
            rows = pl.ds(pl.multiple_of(start + strip * 16, 16), 16)
            for t in range(tiles):
                lanes = pl.ds(t * LANES, LANES)
                blocks[me, rows, lanes] = (mixed[rows, lanes] * factors[t]).astype(jnp.bfloat16)
            return carry

        lax.fori_loop(0, count // 16, body, 0, unroll=2)

    up, down, across, sibling = (0, 1), (0, 3), (1, 0), None
    rows_sent = [0]

    def piece_copy(block, piece, target):
        rows = pl.ds(*PIECES[piece])
        if target is sibling:
            recv = sibling_sem.at[0]
            goal = device(0, 0, 1)
        else:
            recv = recv_sem.at[(block[0] - target[0]) % 2 * 4 + (block[1] - target[1]) % 4, piece]
            goal = device(*target)
        return remote(blocks.at[device(*block), rows, :], send_sem.at[0], recv, rows=goal)

    def send(block, piece, target):
        piece_copy(block, piece, target).start()
        rows_sent[0] += PIECES[piece][1]

    def arrived(block, piece):
        wait_bytes(
            blocks.at[device(*block), pl.ds(*PIECES[piece]), :],
            recv_sem.at[block[0] * 4 + block[1], piece],
        )

    def pass_on(block, piece, *targets):
        arrived(block, piece)
        for target in targets + (sibling,):
            send(block, piece, target)

    own, below, above, far = (0, 0), (0, 3), (0, 1), (0, 2)
    side, side_below, side_above, side_far = (1, 0), (1, 3), (1, 1), (1, 2)
    narrow(0)
    send(own, 0, up)
    narrow(1)
    send(own, 1, down)
    send(own, 1, up)
    send(own, 0, down)
    narrow(2)
    send(own, 2, across)
    send(own, 2, up)
    narrow(3)
    send(own, 3, down)
    send(own, 3, across)
    send(own, 3, up)
    send(own, 2, down)
    for piece in range(4):
        send(own, piece, sibling)

    pass_on(below, 0, up, across)
    for j in range(1, PEERS):

        @pl.when(place + j < PEERS)
        def _():
            image_copy(place + j, place).wait_recv()
            image_copy(place, place + j).start()

    send(own, 0, across)
    send(own, 1, across)
    pass_on(above, 1, down, across)
    pass_on(side, 2, up)
    pass_on(below, 1, across)
    pass_on(above, 0, across)
    pass_on(side, 3, down, up)
    send(side, 2, down)
    pass_on(below, 2, up)
    pass_on(above, 3, down)
    pass_on(side, 0)
    for j in range(1, PEERS):

        @pl.when(place + j >= PEERS)
        def _():
            image_copy(place + j - PEERS, place).wait_recv()

    image = norm_images[0]
    for j in range(1, PEERS):
        image = image + norm_images[j]
    norm_pairs[me] = image
    for j in range(1, DEVICES):
        remote(
            norm_pairs.at[me], pair_sem.at[0], pair_sem.at[1], rows=lax.rem(me + j, DEVICES)
        ).start()

    pass_on(below, 3)
    pass_on(above, 2)
    pass_on(side, 1)
    pass_on(far, 0, across)
    pass_on(far, 1, across)
    pass_on(side_below, 0)
    pass_on(side_above, 1)
    pass_on(side_below, 2, up)
    pass_on(side_above, 3, down)
    pass_on(side_below, 1)
    pass_on(side_below, 3)
    pass_on(side_above, 2)
    pass_on(side_above, 0)
    pass_on(far, 2)
    pass_on(far, 3)
    pass_on(side_far, 0)
    pass_on(side_far, 1)
    pass_on(side_far, 2)
    pass_on(side_far, 3)

    wait_bytes(norm_pairs.at[pl.ds(0, DEVICES - 1)], pair_sem.at[1])
    for j in range(DEVICES // 2):
        norm_all[pl.ds(7 * j, 8), :] = norm_pairs[2 * j] + norm_pairs[2 * j + 1]
    serve[...] = norm_all[pl.ds(0, NORM), :].astype(serve.dtype)
    wait_bytes(sums.at[pl.ds(0, DEVICES - 1)], sum_sem.at[0])
    wait_bytes(norm_images.at[pl.ds(0, PEERS - 1)], image_send.at[0])
    wait_bytes(norm_pairs.at[pl.ds(0, DEVICES - 1)], pair_sem.at[0])

    wait_bytes(blocks.at[pl.ds(0, DEVICES // 2)], sibling_sem.at[0])
    assert rows_sent[0] % depth == 0
    wait_bytes(blocks.at[pl.ds(0, rows_sent[0] // depth)], send_sem.at[0])


def write_kernel(
    blocks,
    scale_query,
    scale_key,
    scale_value,
    serve,
    query,
    key,
    value,
    query_scale,
    key_scale,
    value_scale,
    gains,
    sem,
    small_sem,
):
    depth = blocks.shape[1]
    outs = (query, key, value)
    for b in range(DEVICES):
        at = 0
        for n, out in enumerate(outs):
            pltpu.make_async_copy(
                blocks.at[b, :, pl.ds(at, out.shape[1])],
                out.at[pl.ds(b * depth, depth), :],
                sem.at[n],
            ).start()
            at += out.shape[1]
    small = (
        (scale_query, query_scale),
        (scale_key, key_scale),
        (scale_value, value_scale),
        (serve, gains),
    )
    for i, (source, target) in enumerate(small):
        pltpu.make_async_copy(source, target, small_sem.at[i]).start()
    for n, out in enumerate(outs):
        pltpu.make_async_copy(out, out, sem.at[n]).wait()
    for i, (source, target) in enumerate(small):
        pltpu.make_async_copy(source, target, small_sem.at[i]).wait()


def shards(
    one_query,
    other_query,
    one_key,
    other_key,
    one_value,
    other_value,
    mix_share,
    norm_train,
    norm_step,
):
    f32, bf16 = jnp.float32, jnp.bfloat16
    depth, queries = one_query.shape
    keys = one_key.shape[1]
    wide = queries + 2 * keys
    tall = -(-depth // LANES) * LANES
    dma = pltpu.SemaphoreType.DMA
    hbm, vmem = pl.BlockSpec(memory_space=pltpu.HBM), pl.BlockSpec(memory_space=pltpu.VMEM)
    blocks, scale_query, scale_key, scale_value, serve = pl.pallas_call(
        gather_kernel,
        out_shape=(
            pltpu.VMEM((DEVICES, depth, wide), bf16),
            pltpu.VMEM((queries // LANES, LANES), f32),
            pltpu.VMEM((keys // LANES, LANES), f32),
            pltpu.VMEM((keys // LANES, LANES), f32),
            pltpu.VMEM((NORM, LANES), bf16),
        ),
        in_specs=[hbm] * 9,
        out_specs=[vmem] * 5,
        scratch_shapes=[
            pltpu.VMEM((2, depth, wide), f32),
            pltpu.VMEM((depth, wide), f32),
            pltpu.VMEM((tall, LANES), f32),
            pltpu.VMEM((1, tall), f32),
            pltpu.VMEM((1, depth), f32),
            pltpu.VMEM((1, NORM), f32),
            pltpu.VMEM((1, NORM), f32),
            pltpu.VMEM((DEVICES, 1, wide), f32),
            pltpu.VMEM((1, LANES), f32),
            pltpu.VMEM((PEERS, 8, LANES), f32),
            pltpu.VMEM((DEVICES, 8, LANES), f32),
            pltpu.VMEM((64, LANES), f32),
            dma((LOADS,)),
            dma((3,)),
            dma((1,)),
            dma((8, 4)),
            dma((1,)),
            dma((2,)),
            dma((1,)),
            dma((PEERS,)),
            dma((2,)),
        ],
        compiler_params=pltpu.CompilerParams(
            collective_id=0, has_side_effects=True, vmem_limit_bytes=48 * 1024 * 1024
        ),
        name="gather",
    )(
        one_query,
        other_query,
        one_key,
        other_key,
        one_value,
        other_value,
        mix_share.reshape(1, depth),
        norm_train.reshape(1, NORM),
        norm_step.reshape(1, NORM),
    )
    finals = pl.pallas_call(
        write_kernel,
        out_shape=(
            jax.ShapeDtypeStruct((DEVICES * depth, queries), bf16),
            jax.ShapeDtypeStruct((DEVICES * depth, keys), bf16),
            jax.ShapeDtypeStruct((DEVICES * depth, keys), bf16),
            jax.ShapeDtypeStruct((queries // LANES, LANES), f32),
            jax.ShapeDtypeStruct((keys // LANES, LANES), f32),
            jax.ShapeDtypeStruct((keys // LANES, LANES), f32),
            jax.ShapeDtypeStruct((NORM, LANES), bf16),
        ),
        in_specs=[vmem] * 5,
        out_specs=[hbm] * 7,
        scratch_shapes=[dma((3,)), dma((4,))],
        compiler_params=pltpu.CompilerParams(vmem_limit_bytes=1024 * 1024),
        name="write",
    )(blocks, scale_query, scale_key, scale_value, serve)
    return finals[:3] + tuple(a.reshape(-1) for a in finals[3:])


def solution(mesh):
    in_specs = (
        P("rows", "width"),
        P("rows", "width"),
        P("rows", "width"),
        P("rows", "width"),
        P("rows", "width"),
        P("rows", "width"),
        P("rows"),
        P(("rows", "width")),
        P(("rows", "width")),
    )
    out_specs = (
        P(None, "width"),
        P(None, "width"),
        P(None, "width"),
        P("width"),
        P("width"),
        P("width"),
        P(),
    )
    return jax.shard_map(shards, mesh=mesh, in_specs=in_specs, out_specs=out_specs, check_vma=False)
```

```python
import jax
import jax.numpy as jnp
from jax import lax
from jax.experimental import pallas as pl
from jax.experimental.pallas import tpu as pltpu
from jax.sharding import PartitionSpec as P

MESH = pl.DeviceIdType.MESH
LANES = 128
DEVICES = 16
PEERS = 8
NORM = 56

LOW_UP, LOW_DOWN, HIGH_UP, HIGH_DOWN = (0, 104), (104, 96), (200, 120), (320, 128)
EARLY = 40
LAST_UP = ((200, 40), (240, 48), (288, 32))
LAST_DOWN = ((320, 64), (384, 32), (416, 32))
LAST_ACROSS = ((104, 64), (168, 32))
ARRIVALS = 33
LOADS = 4


def gather_kernel(
    one_query,
    other_query,
    one_key,
    other_key,
    one_value,
    other_value,
    mix,
    train,
    step,
    blocks,
    scale_query,
    scale_key,
    scale_value,
    serve,
    both,
    mixed,
    shares,
    share_row,
    mix_here,
    train_here,
    step_here,
    sums,
    norm_row,
    norm_images,
    norm_pairs,
    norm_all,
    early,
    load_sem,
    small_sem,
    send_sem,
    recv_sem,
    sibling_sem,
    sum_sem,
    image_send,
    image_recv,
    pair_sem,
    early_send,
    early_recv,
):
    depth, wide = mixed.shape
    tiles = wide // LANES
    me = lax.axis_index("rows")
    place = lax.axis_index("width")
    core = lax.rem(me, 2)
    y = lax.rem(lax.div(me, 2), 4)
    z = lax.div(me, 8)

    def device(dz, dy, other=0):
        return lax.rem(z + dz, 2) * 8 + lax.rem(y + dy, 4) * 2 + lax.rem(core + other, 2)

    def remote(ref, send, recv, **target):
        return pltpu.make_async_remote_copy(
            src_ref=ref,
            dst_ref=ref,
            send_sem=send,
            recv_sem=recv,
            device_id=target,
            device_id_type=MESH,
        )

    def wait_bytes(ref, sem):
        pltpu.make_async_copy(ref, ref, sem).wait()

    for i, (source, target) in enumerate(
        ((mix, mix_here), (train, train_here), (step, step_here))
    ):
        pltpu.make_async_copy(source, target, small_sem.at[i]).start()
    chunk = depth // LOADS
    for i in range(LOADS):
        rows = pl.ds(i * chunk, chunk)
        at = 0
        for pair in ((one_query, other_query), (one_key, other_key), (one_value, other_value)):
            for n, source in enumerate(pair):
                columns = pl.ds(at, source.shape[1])
                pltpu.make_async_copy(
                    source.at[rows, :], both.at[n, rows, columns], load_sem.at[i]
                ).start()
            at += pair[0].shape[1]

    barrier = pltpu.get_barrier_semaphore()
    for j in range(1, DEVICES):
        pl.semaphore_signal(
            barrier, inc=1, device_id={"rows": lax.rem(me + j, DEVICES)}, device_id_type=MESH
        )
    for j in range(1, PEERS):

        @pl.when(place + j < PEERS)
        def _():
            pl.semaphore_signal(
                barrier, inc=1, device_id={"width": place + j}, device_id_type=MESH
            )

    for i, target in enumerate((mix_here, train_here, step_here)):
        wait_bytes(target, small_sem.at[i])

    share_row[...] = jnp.zeros_like(share_row)
    share_row[:, pl.ds(0, depth)] = mix_here[...]
    for i in range(shares.shape[0] // LANES):
        row = share_row[:, pl.ds(i * LANES, LANES)]
        shares[pl.ds(i * LANES, LANES), :] = jnp.broadcast_to(row, (LANES, LANES)).T

    norm_row[...] = jnp.zeros_like(norm_row)
    norm_row[:, pl.ds(0, NORM)] = train_here[...] + step_here[...]
    first = (core * PEERS + place) * NORM
    gains = jnp.broadcast_to(norm_row[...], (8, LANES))
    gains = pltpu.roll(gains, lax.rem(first, LANES), 1)
    flat = lax.broadcasted_iota(jnp.int32, (8, LANES), 0) * LANES + lax.broadcasted_iota(
        jnp.int32, (8, LANES), 1
    )
    inside = (flat >= first) & (flat < first + NORM)
    norm_images[place] = jnp.where(inside, gains, 0.0)

    def mix_rows(strip, partial):
        rows = pl.ds(pl.multiple_of(strip * 8, 8), 8)
        share = shares[rows, :]
        rest = 1.0 - share
        found = []
        for t in range(tiles):
            lanes = pl.ds(t * LANES, LANES)
            value = share * both[0, rows, lanes] + rest * both[1, rows, lanes]
            mixed[rows, lanes] = value
            found.append(partial[t] + value * value)
        return tuple(found)

    partial = tuple(jnp.zeros((8, LANES), jnp.float32) for _ in range(tiles))
    for i in range(LOADS):
        wait_bytes(both.at[:, pl.ds(i * chunk, chunk), :], load_sem.at[i])
        partial = lax.fori_loop(i * chunk // 8, (i + 1) * chunk // 8, mix_rows, partial, unroll=2)
    for t in range(tiles):
        sums[me, :, pl.ds(t * LANES, LANES)] = jnp.sum(partial[t], axis=0, keepdims=True)

    pl.semaphore_wait(barrier, DEVICES - 1 + place)

    for j in range(1, DEVICES):
        remote(sums.at[me], sum_sem.at[0], sum_sem.at[1], rows=lax.rem(me + j, DEVICES)).start()

    def image_copy(source, target):
        return remote(norm_images.at[source], image_send.at[0], image_recv.at[source], width=target)

    for j in range(1, PEERS):

        @pl.when(place + j >= PEERS)
        def _():
            image_copy(place, place + j - PEERS).start()

    up, down, across, sibling = (0, 1), (0, 3), (1, 0), None
    early_parts = ((LOW_UP, up), (LOW_DOWN, down), (HIGH_UP, across))
    for n, ((start, _), target) in enumerate(early_parts):
        pltpu.make_async_remote_copy(
            src_ref=mixed.at[pl.ds(start, EARLY), :],
            dst_ref=early.at[n],
            send_sem=early_send.at[0],
            recv_sem=early_recv.at[n],
            device_id={"rows": device(*target)},
            device_id_type=MESH,
        ).start()

    wait_bytes(sums.at[pl.ds(0, DEVICES - 1)], sum_sem.at[1])
    total = sums[0]
    for j in range(1, DEVICES):
        total = total + sums[j]
    scale = jnp.sqrt(total)
    t = 0
    for out in (scale_query, scale_key, scale_value):
        for i in range(out.shape[0]):
            out[i : i + 1, :] = scale[:, t * LANES : (t + 1) * LANES]
            t += 1
    inverse = 1.0 / scale
    factors = [
        jnp.broadcast_to(inverse[:, t * LANES : (t + 1) * LANES], (8, LANES)) for t in range(tiles)
    ]

    def narrow(source, skip, block, start, count):
        def body(strip, carry):
            here = pl.ds(pl.multiple_of(skip + strip * 8, 8), 8)
            there = pl.ds(pl.multiple_of(start + strip * 8, 8), 8)
            for t in range(tiles):
                lanes = pl.ds(t * LANES, LANES)
                blocks[block, there, lanes] = (source[here, lanes] * factors[t]).astype(jnp.bfloat16)
            return carry

        lax.fori_loop(0, count // 8, body, 0, unroll=4)

    rows_sent = [0]
    places = {}

    def arrival(block, part):
        return recv_sem.at[places.setdefault((block, part), len(places))]

    def part_copy(block, part, target):
        rows = pl.ds(*part)
        if target is sibling:
            recv = sibling_sem.at[0]
            goal = device(0, 0, 1)
        else:
            recv = arrival(((block[0] - target[0]) % 2, (block[1] - target[1]) % 4), part)
            goal = device(*target)
        return remote(blocks.at[device(*block), rows, :], send_sem.at[0], recv, rows=goal)

    def send(block, part, *targets):
        for target in targets:
            part_copy(block, part, target).start()
            rows_sent[0] += part[1]

    def arrived(block, part):
        wait_bytes(blocks.at[device(*block), pl.ds(*part), :], arrival(block, part))

    def pass_on(block, part, *targets):
        arrived(block, part)
        send(block, part, *targets, sibling)

    def rest(part):
        return part[0] + EARLY, part[1] - EARLY

    own, below, above, far = (0, 0), (0, 3), (0, 1), (0, 2)
    side, side_below, side_above, side_far = (1, 0), (1, 3), (1, 1), (1, 2)
    for part in (LOW_UP, LOW_DOWN, HIGH_UP, HIGH_DOWN):
        narrow(mixed, part[0], me, *part)
        if part is LOW_UP:
            send(own, rest(LOW_UP), up)
        if part is LOW_DOWN:
            send(own, rest(LOW_DOWN), down)
            send(own, LOW_DOWN, up)
            send(own, LOW_UP, down)
        if part is HIGH_UP:
            send(own, rest(HIGH_UP), across)
            send(own, HIGH_UP, up)
    send(own, HIGH_DOWN, down, across, up)
    send(own, HIGH_UP, down)
    for part in (LOW_UP, LOW_DOWN, HIGH_UP, HIGH_DOWN):
        send(own, part, sibling)
    for n, (block, ((start, _), _)) in enumerate(zip((below, above, side), early_parts)):
        wait_bytes(early.at[n], early_recv.at[n])
        narrow(early.at[n], 0, device(*block), start, EARLY)

    arrived(below, rest(LOW_UP))
    send(below, LOW_UP, up)
    arrived(above, rest(LOW_DOWN))
    send(above, LOW_DOWN, down)
    for j in range(1, PEERS):

        @pl.when(place + j < PEERS)
        def _():
            image_copy(place + j, place).wait_recv()
            image_copy(place, place + j).start()

    send(own, LOW_UP, across)
    send(own, LOW_DOWN, across)
    send(below, LOW_UP, across, sibling)
    send(above, LOW_DOWN, across, sibling)
    arrived(side, rest(HIGH_UP))
    send(side, HIGH_UP, up, sibling)
    pass_on(below, LOW_DOWN, across)
    pass_on(above, LOW_UP, across)
    pass_on(side, HIGH_DOWN, down, up)
    send(side, HIGH_UP, down)
    pass_on(below, HIGH_UP, up)
    pass_on(above, HIGH_DOWN, down)
    pass_on(side, LOW_UP)
    for j in range(1, PEERS):

        @pl.when(place + j >= PEERS)
        def _():
            image_copy(place + j - PEERS, place).wait_recv()

    image = norm_images[0]
    for j in range(1, PEERS):
        image = image + norm_images[j]
    norm_pairs[me] = image
    for j in range(1, DEVICES):
        remote(
            norm_pairs.at[me], pair_sem.at[0], pair_sem.at[1], rows=lax.rem(me + j, DEVICES)
        ).start()

    pass_on(below, HIGH_DOWN)
    pass_on(above, HIGH_UP)
    pass_on(side, LOW_DOWN)
    pass_on(far, LOW_UP, across)
    arrived(far, LOW_DOWN)
    send(far, LOW_DOWN, sibling)
    for part in LAST_ACROSS:
        send(far, part, across)
    pass_on(side_below, LOW_UP)
    pass_on(side_above, LOW_DOWN)
    arrived(side_below, HIGH_UP)
    for part in LAST_UP:
        send(side_below, part, up)
    send(side_below, HIGH_UP, sibling)
    arrived(side_above, HIGH_DOWN)
    for part in LAST_DOWN:
        send(side_above, part, down)
    send(side_above, HIGH_DOWN, sibling)
    pass_on(side_below, LOW_DOWN)
    pass_on(side_below, HIGH_DOWN)
    pass_on(side_above, HIGH_UP)
    pass_on(side_above, LOW_UP)
    pass_on(far, HIGH_UP)
    pass_on(far, HIGH_DOWN)
    pass_on(side_far, LOW_UP)
    for up_part, down_part in zip(LAST_UP[:2], LAST_DOWN[:2]):
        pass_on(side_far, up_part)
        pass_on(side_far, down_part)
    pass_on(side_far, LAST_ACROSS[0])
    pass_on(side_far, LAST_UP[2])
    pass_on(side_far, LAST_DOWN[2])
    pass_on(side_far, LAST_ACROSS[1])
    assert len(places) == ARRIVALS

    wait_bytes(norm_pairs.at[pl.ds(0, DEVICES - 1)], pair_sem.at[1])
    for j in range(DEVICES // 2):
        norm_all[pl.ds(7 * j, 8), :] = norm_pairs[2 * j] + norm_pairs[2 * j + 1]
    serve[...] = norm_all[pl.ds(0, NORM), :].astype(serve.dtype)
    wait_bytes(sums.at[pl.ds(0, DEVICES - 1)], sum_sem.at[0])
    wait_bytes(norm_images.at[pl.ds(0, PEERS - 1)], image_send.at[0])
    wait_bytes(norm_pairs.at[pl.ds(0, DEVICES - 1)], pair_sem.at[0])

    wait_bytes(early, early_send.at[0])
    wait_bytes(blocks.at[pl.ds(0, DEVICES // 2)], sibling_sem.at[0])
    count = -(-rows_sent[0] // depth)
    assert rows_sent[0] % (count * 8) == 0
    wait_bytes(blocks.at[pl.ds(0, count), pl.ds(0, rows_sent[0] // count), :], send_sem.at[0])


def write_kernel(
    blocks,
    scale_query,
    scale_key,
    scale_value,
    serve,
    query,
    key,
    value,
    query_scale,
    key_scale,
    value_scale,
    gains,
    sem,
    small_sem,
):
    depth = blocks.shape[1]
    outs = (query, key, value)
    for b in range(DEVICES):
        at = 0
        for n, out in enumerate(outs):
            pltpu.make_async_copy(
                blocks.at[b, :, pl.ds(at, out.shape[1])],
                out.at[pl.ds(b * depth, depth), :],
                sem.at[n],
            ).start()
            at += out.shape[1]
    small = (
        (scale_query, query_scale),
        (scale_key, key_scale),
        (scale_value, value_scale),
        (serve, gains),
    )
    for i, (source, target) in enumerate(small):
        pltpu.make_async_copy(source, target, small_sem.at[i]).start()
    for n, out in enumerate(outs):
        pltpu.make_async_copy(out, out, sem.at[n]).wait()
    for i, (source, target) in enumerate(small):
        pltpu.make_async_copy(source, target, small_sem.at[i]).wait()


def shards(
    one_query,
    other_query,
    one_key,
    other_key,
    one_value,
    other_value,
    mix_share,
    norm_train,
    norm_step,
):
    f32, bf16 = jnp.float32, jnp.bfloat16
    depth, queries = one_query.shape
    keys = one_key.shape[1]
    wide = queries + 2 * keys
    tall = -(-depth // LANES) * LANES
    dma = pltpu.SemaphoreType.DMA
    hbm, vmem = pl.BlockSpec(memory_space=pltpu.HBM), pl.BlockSpec(memory_space=pltpu.VMEM)
    blocks, scale_query, scale_key, scale_value, serve = pl.pallas_call(
        gather_kernel,
        out_shape=(
            pltpu.VMEM((DEVICES, depth, wide), bf16),
            pltpu.VMEM((queries // LANES, LANES), f32),
            pltpu.VMEM((keys // LANES, LANES), f32),
            pltpu.VMEM((keys // LANES, LANES), f32),
            pltpu.VMEM((NORM, LANES), bf16),
        ),
        in_specs=[hbm] * 9,
        out_specs=[vmem] * 5,
        scratch_shapes=[
            pltpu.VMEM((2, depth, wide), f32),
            pltpu.VMEM((depth, wide), f32),
            pltpu.VMEM((tall, LANES), f32),
            pltpu.VMEM((1, tall), f32),
            pltpu.VMEM((1, depth), f32),
            pltpu.VMEM((1, NORM), f32),
            pltpu.VMEM((1, NORM), f32),
            pltpu.VMEM((DEVICES, 1, wide), f32),
            pltpu.VMEM((1, LANES), f32),
            pltpu.VMEM((PEERS, 8, LANES), f32),
            pltpu.VMEM((DEVICES, 8, LANES), f32),
            pltpu.VMEM((64, LANES), f32),
            pltpu.VMEM((3, EARLY, wide), f32),
            dma((LOADS,)),
            dma((3,)),
            dma((1,)),
            dma((ARRIVALS,)),
            dma((1,)),
            dma((2,)),
            dma((1,)),
            dma((PEERS,)),
            dma((2,)),
            dma((1,)),
            dma((3,)),
        ],
        compiler_params=pltpu.CompilerParams(
            collective_id=0, has_side_effects=True, vmem_limit_bytes=48 * 1024 * 1024
        ),
        name="gather",
    )(
        one_query,
        other_query,
        one_key,
        other_key,
        one_value,
        other_value,
        mix_share.reshape(1, depth),
        norm_train.reshape(1, NORM),
        norm_step.reshape(1, NORM),
    )
    finals = pl.pallas_call(
        write_kernel,
        out_shape=(
            jax.ShapeDtypeStruct((DEVICES * depth, queries), bf16),
            jax.ShapeDtypeStruct((DEVICES * depth, keys), bf16),
            jax.ShapeDtypeStruct((DEVICES * depth, keys), bf16),
            jax.ShapeDtypeStruct((queries // LANES, LANES), f32),
            jax.ShapeDtypeStruct((keys // LANES, LANES), f32),
            jax.ShapeDtypeStruct((keys // LANES, LANES), f32),
            jax.ShapeDtypeStruct((NORM, LANES), bf16),
        ),
        in_specs=[vmem] * 5,
        out_specs=[hbm] * 7,
        scratch_shapes=[dma((3,)), dma((4,))],
        compiler_params=pltpu.CompilerParams(vmem_limit_bytes=1024 * 1024),
        name="write",
    )(blocks, scale_query, scale_key, scale_value, serve)
    return finals[:3] + tuple(a.reshape(-1) for a in finals[3:])


def solution(mesh):
    in_specs = (
        P("rows", "width"),
        P("rows", "width"),
        P("rows", "width"),
        P("rows", "width"),
        P("rows", "width"),
        P("rows", "width"),
        P("rows"),
        P(("rows", "width")),
        P(("rows", "width")),
    )
    out_specs = (
        P(None, "width"),
        P(None, "width"),
        P(None, "width"),
        P("width"),
        P("width"),
        P("width"),
        P(),
    )
    return jax.shard_map(shards, mesh=mesh, in_specs=in_specs, out_specs=out_specs, check_vma=False)
```

```python
import jax
import jax.numpy as jnp
from jax import lax
from jax.experimental import pallas as pl
from jax.experimental.pallas import tpu as pltpu
from jax.sharding import PartitionSpec as P

MESH = pl.DeviceIdType.MESH
LANES = 128
DEVICES = 16
CHIPS = 8
PEERS = 8
NORM = 56

LOW_UP, LOW_DOWN, HIGH_UP, HIGH_DOWN = (0, 104), (104, 96), (200, 120), (320, 128)
EARLY = 40
LAST_UP = ((200, 40), (240, 48), (288, 32))
LAST_DOWN = ((320, 64), (384, 32), (416, 32))
LAST_ACROSS = ((104, 64), (168, 32))
ARRIVALS = 33
LOADS = 4


def gather_kernel(
    one_query,
    other_query,
    one_key,
    other_key,
    one_value,
    other_value,
    mix,
    train,
    step,
    blocks,
    scale_query,
    scale_key,
    scale_value,
    serve,
    both,
    mixed,
    shares,
    share_row,
    mix_here,
    train_here,
    step_here,
    sums,
    halves,
    norm_rows,
    norm_images,
    norm_all,
    early,
    load_sem,
    small_sem,
    send_sem,
    recv_sem,
    sibling_sem,
    sum_sem,
    half_sem,
    row_send,
    row_recv,
    image_sem,
    both_sem,
    early_send,
    early_recv,
):
    depth, wide = mixed.shape
    tiles = wide // LANES
    me = lax.axis_index("rows")
    place = lax.axis_index("width")
    core = lax.rem(me, 2)
    y = lax.rem(lax.div(me, 2), 4)
    z = lax.div(me, 8)
    chip = lax.div(me, 2)

    def device(dz, dy, other=0):
        return lax.rem(z + dz, 2) * 8 + lax.rem(y + dy, 4) * 2 + lax.rem(core + other, 2)

    def remote(ref, send, recv, **target):
        return pltpu.make_async_remote_copy(
            src_ref=ref,
            dst_ref=ref,
            send_sem=send,
            recv_sem=recv,
            device_id=target,
            device_id_type=MESH,
        )

    def wait_bytes(ref, sem):
        pltpu.make_async_copy(ref, ref, sem).wait()

    chunk = depth // LOADS

    def load(i):
        rows = pl.ds(i * chunk, chunk)
        at = 0
        for pair in ((one_query, other_query), (one_key, other_key), (one_value, other_value)):
            for n, source in enumerate(pair):
                columns = pl.ds(at, source.shape[1])
                pltpu.make_async_copy(
                    source.at[rows, :], both.at[n, rows, columns], load_sem.at[i]
                ).start()
            at += pair[0].shape[1]

    load(0)
    for i, (source, target) in enumerate(
        ((mix, mix_here), (train, train_here), (step, step_here))
    ):
        pltpu.make_async_copy(source, target, small_sem.at[i]).start()
    barrier = pltpu.get_barrier_semaphore()
    for j in range(1, DEVICES):
        pl.semaphore_signal(
            barrier, inc=1, device_id={"rows": lax.rem(me + j, DEVICES)}, device_id_type=MESH
        )
    for j in range(1, PEERS):

        @pl.when(place + j < PEERS)
        def _():
            pl.semaphore_signal(
                barrier, inc=1, device_id={"width": place + j}, device_id_type=MESH
            )

    for i in range(1, LOADS):
        load(i)

    for i, target in enumerate((mix_here, train_here, step_here)):
        wait_bytes(target, small_sem.at[i])

    share_row[...] = jnp.zeros_like(share_row)
    share_row[:, pl.ds(0, depth)] = mix_here[...]
    for i in range(shares.shape[0] // LANES):
        row = share_row[:, pl.ds(i * LANES, LANES)]
        shares[pl.ds(i * LANES, LANES), :] = jnp.broadcast_to(row, (LANES, LANES)).T

    norm_rows[place] = jnp.zeros((1, LANES), jnp.float32)
    norm_rows[place, :, pl.ds(0, NORM)] = train_here[...] + step_here[...]

    def mix_rows(strip, partial):
        rows = pl.ds(pl.multiple_of(strip * 8, 8), 8)
        share = shares[rows, :]
        rest = 1.0 - share
        found = []
        for t in range(tiles):
            lanes = pl.ds(t * LANES, LANES)
            value = share * both[0, rows, lanes] + rest * both[1, rows, lanes]
            mixed[rows, lanes] = value
            found.append(partial[t] + value * value)
        return tuple(found)

    partial = tuple(jnp.zeros((8, LANES), jnp.float32) for _ in range(tiles))
    for i in range(LOADS):
        wait_bytes(both.at[:, pl.ds(i * chunk, chunk), :], load_sem.at[i])
        partial = lax.fori_loop(i * chunk // 8, (i + 1) * chunk // 8, mix_rows, partial, unroll=2)
    for t in range(tiles):
        sums[chip, :, pl.ds(t * LANES, LANES)] = jnp.sum(partial[t], axis=0, keepdims=True)

    pl.semaphore_wait(barrier, DEVICES - 1 + place)

    others = ((1, 2), (1, 1), (1, 3), (0, 2), (1, 0), (0, 1), (0, 3))
    for dz, dy in others:
        remote(sums.at[chip], sum_sem.at[0], sum_sem.at[1], rows=device(dz, dy)).start()

    def row_copy(source, target):
        return remote(norm_rows.at[source], row_send.at[0], row_recv.at[source], width=target)

    for j in range(1, PEERS):

        @pl.when(place + j >= PEERS)
        def _():
            row_copy(place, place + j - PEERS).start()

    up, down, across, sibling = (0, 1), (0, 3), (1, 0), None
    early_parts = ((LOW_UP, up), (LOW_DOWN, down), (HIGH_UP, across))
    for n, ((start, _), target) in enumerate(early_parts):
        pltpu.make_async_remote_copy(
            src_ref=mixed.at[pl.ds(start, EARLY), :],
            dst_ref=early.at[n],
            send_sem=early_send.at[0],
            recv_sem=early_recv.at[n],
            device_id={"rows": device(*target)},
            device_id_type=MESH,
        ).start()

    wait_bytes(sums.at[pl.ds(0, CHIPS - 1)], sum_sem.at[1])
    half = sums[0]
    for j in range(1, CHIPS):
        half = half + sums[j]
    halves[core] = half
    remote(halves.at[core], half_sem.at[0], half_sem.at[1], rows=device(0, 0, 1)).start()
    wait_bytes(halves.at[0], half_sem.at[1])
    total = halves[0] + halves[1]
    scale = jnp.sqrt(total)
    t = 0
    for out in (scale_query, scale_key, scale_value):
        for i in range(out.shape[0]):
            out[i : i + 1, :] = scale[:, t * LANES : (t + 1) * LANES]
            t += 1
    inverse = 1.0 / scale
    factors = [
        jnp.broadcast_to(inverse[:, t * LANES : (t + 1) * LANES], (8, LANES)) for t in range(tiles)
    ]

    def narrow(source, skip, block, start, count):
        def body(strip, carry):
            here = pl.ds(pl.multiple_of(skip + strip * 8, 8), 8)
            there = pl.ds(pl.multiple_of(start + strip * 8, 8), 8)
            for t in range(tiles):
                lanes = pl.ds(t * LANES, LANES)
                blocks[block, there, lanes] = (source[here, lanes] * factors[t]).astype(jnp.bfloat16)
            return carry

        lax.fori_loop(0, count // 8, body, 0, unroll=4)

    rows_sent = [0]
    places = {}

    def arrival(block, part):
        return recv_sem.at[places.setdefault((block, part), len(places))]

    def part_copy(block, part, target):
        rows = pl.ds(*part)
        if target is sibling:
            return remote(
                blocks.at[device(*block), rows, :],
                send_sem.at[1],
                sibling_sem.at[0],
                rows=device(0, 0, 1),
            )
        there = ((block[0] - target[0]) % 2, (block[1] - target[1]) % 4)
        return remote(
            blocks.at[device(*block), rows, :],
            send_sem.at[0],
            arrival(there, part),
            rows=device(*target),
        )

    def send(block, part, *targets):
        for target in targets:
            part_copy(block, part, target).start()
            if target is not sibling:
                rows_sent[0] += part[1]

    def arrived(block, part):
        wait_bytes(blocks.at[device(*block), pl.ds(*part), :], arrival(block, part))

    def pass_on(block, part, *targets):
        arrived(block, part)
        send(block, part, *targets, sibling)

    def rest(part):
        return part[0] + EARLY, part[1] - EARLY

    own, below, above, far = (0, 0), (0, 3), (0, 1), (0, 2)
    side, side_below, side_above, side_far = (1, 0), (1, 3), (1, 1), (1, 2)
    for part in (LOW_UP, LOW_DOWN, HIGH_UP, HIGH_DOWN):
        narrow(mixed, part[0], me, *part)
        if part is LOW_UP:
            send(own, rest(LOW_UP), up)
        if part is LOW_DOWN:
            send(own, rest(LOW_DOWN), down)
            send(own, LOW_DOWN, up)
            send(own, LOW_UP, down)
        if part is HIGH_UP:
            send(own, rest(HIGH_UP), across)
            send(own, HIGH_UP, up)
    send(own, HIGH_DOWN, down, across, up)
    send(own, HIGH_UP, down)
    for part in (LOW_UP, LOW_DOWN, HIGH_UP, HIGH_DOWN):
        send(own, part, sibling)
    for n, (block, ((start, _), _)) in enumerate(zip((below, above, side), early_parts)):
        wait_bytes(early.at[n], early_recv.at[n])
        narrow(early.at[n], 0, device(*block), start, EARLY)

    arrived(below, rest(LOW_UP))
    send(below, LOW_UP, up)
    arrived(above, rest(LOW_DOWN))
    send(above, LOW_DOWN, down)
    for j in range(1, PEERS):

        @pl.when(place + j < PEERS)
        def _():
            row_copy(place + j, place).wait_recv()
            row_copy(place, place + j).start()

    send(own, LOW_UP, across)
    send(own, LOW_DOWN, across)
    send(below, LOW_UP, across, sibling)
    send(above, LOW_DOWN, across, sibling)
    arrived(side, rest(HIGH_UP))
    send(side, HIGH_UP, up, sibling)
    pass_on(below, LOW_DOWN, across)
    pass_on(above, LOW_UP, across)
    pass_on(side, HIGH_DOWN, down, up)
    send(side, HIGH_UP, down)
    pass_on(below, HIGH_UP, up)
    pass_on(above, HIGH_DOWN, down)
    pass_on(side, LOW_UP)
    for j in range(1, PEERS):

        @pl.when(place + j >= PEERS)
        def _():
            row_copy(place + j - PEERS, place).wait_recv()

    flat = lax.broadcasted_iota(jnp.int32, (8, LANES), 0) * LANES + lax.broadcasted_iota(
        jnp.int32, (8, LANES), 1
    )
    image = jnp.zeros((8, LANES), jnp.float32)
    for j in range(PEERS):
        first = (core * PEERS + j) * NORM
        gains = pltpu.roll(jnp.broadcast_to(norm_rows[j], (8, LANES)), lax.rem(first, LANES), 1)
        image = jnp.where((flat >= first) & (flat < first + NORM), gains, image)
    norm_images[core, chip] = image.astype(jnp.bfloat16)
    for dz, dy in others:
        remote(
            norm_images.at[core, chip], image_sem.at[0], image_sem.at[1], rows=device(dz, dy)
        ).start()

    pass_on(below, HIGH_DOWN)
    pass_on(above, HIGH_UP)
    pass_on(side, LOW_DOWN)
    pass_on(far, LOW_UP, across)
    arrived(far, LOW_DOWN)
    send(far, LOW_DOWN, sibling)
    for part in LAST_ACROSS:
        send(far, part, across)
    pass_on(side_below, LOW_UP)
    pass_on(side_above, LOW_DOWN)
    arrived(side_below, HIGH_UP)
    for part in LAST_UP:
        send(side_below, part, up)
    send(side_below, HIGH_UP, sibling)
    arrived(side_above, HIGH_DOWN)
    for part in LAST_DOWN:
        send(side_above, part, down)
    send(side_above, HIGH_DOWN, sibling)
    pass_on(side_below, LOW_DOWN)
    pass_on(side_below, HIGH_DOWN)
    pass_on(side_above, HIGH_UP)
    pass_on(side_above, LOW_UP)
    pass_on(far, HIGH_UP)
    pass_on(far, HIGH_DOWN)
    wait_bytes(norm_images.at[0, pl.ds(0, CHIPS - 1)], image_sem.at[1])
    remote(norm_images.at[core], both_sem.at[0], both_sem.at[1], rows=device(0, 0, 1)).start()
    pass_on(side_far, LOW_UP)
    for up_part, down_part in zip(LAST_UP[:2], LAST_DOWN[:2]):
        pass_on(side_far, up_part)
        pass_on(side_far, down_part)
    pass_on(side_far, LAST_ACROSS[0])
    pass_on(side_far, LAST_UP[2])
    pass_on(side_far, LAST_DOWN[2])
    pass_on(side_far, LAST_ACROSS[1])
    assert len(places) == ARRIVALS

    wait_bytes(norm_images.at[0], both_sem.at[1])
    for j in range(CHIPS):
        norm_all[pl.ds(7 * j, 8), :] = norm_images[0, j].astype(jnp.float32) + norm_images[
            1, j
        ].astype(jnp.float32)
    serve[...] = norm_all[pl.ds(0, NORM), :].astype(serve.dtype)
    wait_bytes(sums.at[pl.ds(0, CHIPS - 1)], sum_sem.at[0])
    wait_bytes(halves.at[0], half_sem.at[0])
    wait_bytes(norm_rows.at[pl.ds(0, PEERS - 1)], row_send.at[0])
    wait_bytes(norm_images.at[0, pl.ds(0, CHIPS - 1)], image_sem.at[0])
    wait_bytes(norm_images.at[0], both_sem.at[0])
    wait_bytes(early, early_send.at[0])
    wait_bytes(blocks.at[pl.ds(0, DEVICES // 2)], sibling_sem.at[0])
    strips = rows_sent[0] // 8
    count = next(n for n in range(1, DEVICES + 1) if strips % n == 0 and strips // n <= depth // 8)
    wait_bytes(blocks.at[pl.ds(0, count), pl.ds(0, strips // count * 8), :], send_sem.at[0])
    wait_bytes(blocks.at[pl.ds(0, DEVICES // 2)], send_sem.at[1])


def write_kernel(
    blocks,
    scale_query,
    scale_key,
    scale_value,
    serve,
    query,
    key,
    value,
    query_scale,
    key_scale,
    value_scale,
    gains,
    sem,
    small_sem,
):
    depth = blocks.shape[1]
    outs = (query, key, value)
    for b in range(DEVICES):
        at = 0
        for n, out in enumerate(outs):
            pltpu.make_async_copy(
                blocks.at[b, :, pl.ds(at, out.shape[1])],
                out.at[pl.ds(b * depth, depth), :],
                sem.at[n],
            ).start()
            at += out.shape[1]
    small = (
        (scale_query, query_scale),
        (scale_key, key_scale),
        (scale_value, value_scale),
        (serve, gains),
    )
    for i, (source, target) in enumerate(small):
        pltpu.make_async_copy(source, target, small_sem.at[i]).start()
    for n, out in enumerate(outs):
        pltpu.make_async_copy(out, out, sem.at[n]).wait()
    for i, (source, target) in enumerate(small):
        pltpu.make_async_copy(source, target, small_sem.at[i]).wait()


def shards(
    one_query,
    other_query,
    one_key,
    other_key,
    one_value,
    other_value,
    mix_share,
    norm_train,
    norm_step,
):
    f32, bf16 = jnp.float32, jnp.bfloat16
    depth, queries = one_query.shape
    keys = one_key.shape[1]
    wide = queries + 2 * keys
    tall = -(-depth // LANES) * LANES
    dma = pltpu.SemaphoreType.DMA
    hbm, vmem = pl.BlockSpec(memory_space=pltpu.HBM), pl.BlockSpec(memory_space=pltpu.VMEM)
    blocks, scale_query, scale_key, scale_value, serve = pl.pallas_call(
        gather_kernel,
        out_shape=(
            pltpu.VMEM((DEVICES, depth, wide), bf16),
            pltpu.VMEM((queries // LANES, LANES), f32),
            pltpu.VMEM((keys // LANES, LANES), f32),
            pltpu.VMEM((keys // LANES, LANES), f32),
            pltpu.VMEM((NORM, LANES), bf16),
        ),
        in_specs=[hbm] * 9,
        out_specs=[vmem] * 5,
        scratch_shapes=[
            pltpu.VMEM((2, depth, wide), f32),
            pltpu.VMEM((depth, wide), f32),
            pltpu.VMEM((tall, LANES), f32),
            pltpu.VMEM((1, tall), f32),
            pltpu.VMEM((1, depth), f32),
            pltpu.VMEM((1, NORM), f32),
            pltpu.VMEM((1, NORM), f32),
            pltpu.VMEM((CHIPS, 1, wide), f32),
            pltpu.VMEM((2, 1, wide), f32),
            pltpu.VMEM((PEERS, 1, LANES), f32),
            pltpu.VMEM((2, CHIPS, 8, LANES), bf16),
            pltpu.VMEM((64, LANES), f32),
            pltpu.VMEM((3, EARLY, wide), f32),
            dma((LOADS,)),
            dma((3,)),
            dma((2,)),
            dma((ARRIVALS,)),
            dma((1,)),
            dma((2,)),
            dma((2,)),
            dma((1,)),
            dma((PEERS,)),
            dma((2,)),
            dma((2,)),
            dma((1,)),
            dma((3,)),
        ],
        compiler_params=pltpu.CompilerParams(
            collective_id=0, has_side_effects=True, vmem_limit_bytes=48 * 1024 * 1024
        ),
        name="gather",
    )(
        one_query,
        other_query,
        one_key,
        other_key,
        one_value,
        other_value,
        mix_share.reshape(1, depth),
        norm_train.reshape(1, NORM),
        norm_step.reshape(1, NORM),
    )
    finals = pl.pallas_call(
        write_kernel,
        out_shape=(
            jax.ShapeDtypeStruct((DEVICES * depth, queries), bf16),
            jax.ShapeDtypeStruct((DEVICES * depth, keys), bf16),
            jax.ShapeDtypeStruct((DEVICES * depth, keys), bf16),
            jax.ShapeDtypeStruct((queries // LANES, LANES), f32),
            jax.ShapeDtypeStruct((keys // LANES, LANES), f32),
            jax.ShapeDtypeStruct((keys // LANES, LANES), f32),
            jax.ShapeDtypeStruct((NORM, LANES), bf16),
        ),
        in_specs=[vmem] * 5,
        out_specs=[hbm] * 7,
        scratch_shapes=[dma((3,)), dma((4,))],
        compiler_params=pltpu.CompilerParams(vmem_limit_bytes=1024 * 1024),
        name="write",
    )(blocks, scale_query, scale_key, scale_value, serve)
    return finals[:3] + tuple(a.reshape(-1) for a in finals[3:])


def solution(mesh):
    in_specs = (
        P("rows", "width"),
        P("rows", "width"),
        P("rows", "width"),
        P("rows", "width"),
        P("rows", "width"),
        P("rows", "width"),
        P("rows"),
        P(("rows", "width")),
        P(("rows", "width")),
    )
    out_specs = (
        P(None, "width"),
        P(None, "width"),
        P(None, "width"),
        P("width"),
        P("width"),
        P("width"),
        P(),
    )
    return jax.shard_map(shards, mesh=mesh, in_specs=in_specs, out_specs=out_specs, check_vma=False)
```

```python
import jax
import jax.numpy as jnp
from jax import lax
from jax.experimental import pallas as pl
from jax.experimental.pallas import tpu as pltpu
from jax.sharding import PartitionSpec as P

MESH = pl.DeviceIdType.MESH
LANES = 128
DEVICES = 16
CHIPS = 8
PEERS = 8
NORM = 56

LOW_UP, LOW_DOWN, HIGH_UP, HIGH_DOWN = (0, 104), (104, 96), (200, 120), (320, 128)
EARLY = 40
LAST_UP = ((200, 40), (240, 48), (288, 16))
LAST_DOWN = ((320, 64), (384, 32), (416, 16))
LAST_ACROSS = ((104, 64), (168, 16))
LENT_UP, LENT_DOWN, LENT_ACROSS = (304, 16), (432, 16), (184, 16)


def rest(part):
    return part[0] + EARLY, part[1] - EARLY


BELOW, ABOVE, FAR = (0, 3), (0, 1), (0, 2)
SIDE, SIDE_BELOW, SIDE_ABOVE, SIDE_FAR = (1, 0), (1, 3), (1, 1), (1, 2)
ARRIVALS = (
    ((BELOW, rest(LOW_UP)), (ABOVE, rest(LOW_DOWN))),
    ((SIDE, rest(HIGH_UP)),),
    ((BELOW, LOW_DOWN), (ABOVE, LOW_UP)),
    ((SIDE, HIGH_DOWN),),
    ((BELOW, HIGH_UP), (ABOVE, HIGH_DOWN)),
    ((BELOW, HIGH_DOWN), (ABOVE, HIGH_UP), (SIDE, LOW_UP), (SIDE, LOW_DOWN)),
    ((FAR, LOW_UP), (FAR, LOW_DOWN)),
    ((SIDE_BELOW, HIGH_UP), (SIDE_ABOVE, HIGH_DOWN)),
    (
        (SIDE_BELOW, LOW_UP),
        (SIDE_BELOW, LOW_DOWN),
        (SIDE_BELOW, HIGH_DOWN),
        (SIDE_ABOVE, HIGH_UP),
    ),
    ((SIDE_ABOVE, LOW_UP), (SIDE_ABOVE, LOW_DOWN), (FAR, HIGH_UP), (FAR, HIGH_DOWN)),
    ((SIDE_FAR, LOW_UP),),
    ((SIDE_FAR, LAST_UP[0]), (SIDE_FAR, LAST_DOWN[0])),
    ((SIDE_FAR, LAST_UP[1]), (SIDE_FAR, LAST_DOWN[1])),
    ((SIDE_FAR, LAST_ACROSS[0]),),
    ((SIDE_FAR, LAST_UP[2]), (SIDE_FAR, LAST_DOWN[2])),
    ((SIDE_FAR, LAST_ACROSS[1]),),
    ((SIDE_FAR, LENT_UP), (SIDE_FAR, LENT_DOWN)),
    ((SIDE_FAR, LENT_ACROSS),),
)
OWN_LENT = len(ARRIVALS) - 2
SIBLING_LENT = len(ARRIVALS)
LOADS = 4


def gather_kernel(
    one_query,
    other_query,
    one_key,
    other_key,
    one_value,
    other_value,
    mix,
    train,
    step,
    blocks,
    scale_query,
    scale_key,
    scale_value,
    serve,
    both,
    mixed,
    shares,
    share_row,
    mix_here,
    train_here,
    step_here,
    sums,
    halves,
    norm_rows,
    norm_images,
    norm_all,
    early,
    load_sem,
    small_sem,
    send_sem,
    recv_sem,
    sibling_sem,
    sum_sem,
    half_sem,
    row_send,
    row_recv,
    image_sem,
    both_sem,
    early_send,
    early_recv,
):
    depth, wide = mixed.shape
    tiles = wide // LANES
    me = lax.axis_index("rows")
    place = lax.axis_index("width")
    core = lax.rem(me, 2)
    y = lax.rem(lax.div(me, 2), 4)
    z = lax.div(me, 8)
    chip = lax.div(me, 2)

    def device(dz, dy, other=0):
        return lax.rem(z + dz, 2) * 8 + lax.rem(y + dy, 4) * 2 + lax.rem(core + other, 2)

    def remote(ref, send, recv, **target):
        return pltpu.make_async_remote_copy(
            src_ref=ref,
            dst_ref=ref,
            send_sem=send,
            recv_sem=recv,
            device_id=target,
            device_id_type=MESH,
        )

    def wait_bytes(ref, sem):
        pltpu.make_async_copy(ref, ref, sem).wait()

    chunk = depth // LOADS

    def load(i):
        rows = pl.ds(i * chunk, chunk)
        at = 0
        for pair in ((one_query, other_query), (one_key, other_key), (one_value, other_value)):
            for n, source in enumerate(pair):
                columns = pl.ds(at, source.shape[1])
                pltpu.make_async_copy(
                    source.at[rows, :], both.at[n, rows, columns], load_sem.at[i]
                ).start()
            at += pair[0].shape[1]

    load(0)
    for i, (source, target) in enumerate(
        ((mix, mix_here), (train, train_here), (step, step_here))
    ):
        pltpu.make_async_copy(source, target, small_sem.at[i]).start()
    barrier = pltpu.get_barrier_semaphore()
    for j in range(1, DEVICES):
        pl.semaphore_signal(
            barrier, inc=1, device_id={"rows": lax.rem(me + j, DEVICES)}, device_id_type=MESH
        )
    for j in range(1, PEERS):

        @pl.when(place + j < PEERS)
        def _():
            pl.semaphore_signal(
                barrier, inc=1, device_id={"width": place + j}, device_id_type=MESH
            )

    for i in range(1, LOADS):
        load(i)

    for i, target in enumerate((mix_here, train_here, step_here)):
        wait_bytes(target, small_sem.at[i])

    share_row[...] = jnp.zeros_like(share_row)
    share_row[:, pl.ds(0, depth)] = mix_here[...]
    for i in range(shares.shape[0] // LANES):
        row = share_row[:, pl.ds(i * LANES, LANES)]
        shares[pl.ds(i * LANES, LANES), :] = jnp.broadcast_to(row, (LANES, LANES)).T

    norm_rows[place] = jnp.zeros((1, LANES), jnp.float32)
    norm_rows[place, :, pl.ds(0, NORM)] = train_here[...] + step_here[...]

    def mix_rows(strip, partial):
        rows = pl.ds(pl.multiple_of(strip * 8, 8), 8)
        share = shares[rows, :]
        rest = 1.0 - share
        found = []
        for t in range(tiles):
            lanes = pl.ds(t * LANES, LANES)
            value = share * both[0, rows, lanes] + rest * both[1, rows, lanes]
            mixed[rows, lanes] = value
            found.append(partial[t] + value * value)
        return tuple(found)

    partial = tuple(jnp.zeros((8, LANES), jnp.float32) for _ in range(tiles))
    for i in range(LOADS):
        wait_bytes(both.at[:, pl.ds(i * chunk, chunk), :], load_sem.at[i])
        partial = lax.fori_loop(i * chunk // 8, (i + 1) * chunk // 8, mix_rows, partial, unroll=2)
    for t in range(tiles):
        sums[chip, :, pl.ds(t * LANES, LANES)] = jnp.sum(partial[t], axis=0, keepdims=True)

    pl.semaphore_wait(barrier, DEVICES - 1 + place)

    others = ((1, 2), (1, 1), (1, 3), (0, 2), (1, 0), (0, 1), (0, 3))
    for dz, dy in others:
        remote(sums.at[chip], sum_sem.at[0], sum_sem.at[1], rows=device(dz, dy)).start()

    def row_copy(source, target):
        return remote(norm_rows.at[source], row_send.at[0], row_recv.at[source], width=target)

    for j in range(1, PEERS):

        @pl.when(place + j >= PEERS)
        def _():
            row_copy(place, place + j - PEERS).start()

    up, down, across = (0, 1), (0, 3), (1, 0)
    early_parts = ((LOW_UP, up), (LOW_DOWN, down), (HIGH_UP, across))
    for n, (part, target) in enumerate(early_parts):
        pltpu.make_async_remote_copy(
            src_ref=mixed.at[pl.ds(part[0], EARLY), :],
            dst_ref=early.at[n],
            send_sem=early_send.at[0],
            recv_sem=early_recv.at[n],
            device_id={"rows": device(*target)},
            device_id_type=MESH,
        ).start()

    wait_bytes(sums.at[pl.ds(0, CHIPS - 1)], sum_sem.at[1])
    half = sums[0]
    for j in range(1, CHIPS):
        half = half + sums[j]
    halves[core] = half
    remote(halves.at[core], half_sem.at[0], half_sem.at[1], rows=device(0, 0, 1)).start()
    wait_bytes(halves.at[0], half_sem.at[1])
    total = halves[0] + halves[1]
    scale = jnp.sqrt(total)
    t = 0
    for out in (scale_query, scale_key, scale_value):
        for i in range(out.shape[0]):
            out[i : i + 1, :] = scale[:, t * LANES : (t + 1) * LANES]
            t += 1
    inverse = 1.0 / scale
    factors = [
        jnp.broadcast_to(inverse[:, t * LANES : (t + 1) * LANES], (8, LANES)) for t in range(tiles)
    ]

    def narrow(source, skip, block, start, count):
        def body(strip, carry):
            here = pl.ds(pl.multiple_of(skip + strip * 8, 8), 8)
            there = pl.ds(pl.multiple_of(start + strip * 8, 8), 8)
            for t in range(tiles):
                lanes = pl.ds(t * LANES, LANES)
                blocks[block, there, lanes] = (source[here, lanes] * factors[t]).astype(jnp.bfloat16)
            return carry

        lax.fori_loop(0, count // 8, body, 0, unroll=4)

    rows_sent = {}

    def start(source, part, send_by, recv, goal):
        remote(
            blocks.at[source, pl.ds(*part), :], send_sem.at[send_by], recv, rows=goal
        ).start()
        rows_sent[send_by] = rows_sent.get(send_by, 0) + part[1]

    line_of = {arrival: n for n, line in enumerate(ARRIVALS) for arrival in line}

    def send(block, part, *targets):
        for target in targets:
            line = line_of[((block[0] - target[0]) % 2, (block[1] - target[1]) % 4), part]
            start(device(*block), part, 0, recv_sem.at[line], device(*target))

    def share(block, part, recv=1):
        start(device(*block), part, 1, sibling_sem.at[recv], device(0, 0, 1))

    def wait_rows(count, sem):
        strips = count // 8
        n = next(n for n in range(1, DEVICES + 1) if strips % n == 0 and strips // n <= depth // 8)
        wait_bytes(blocks.at[pl.ds(0, n), pl.ds(0, strips // n * 8), :], sem)

    def arrived(line):
        wait_rows(sum(part[1] for _, part in ARRIVALS[line]), recv_sem.at[line])

    own = (0, 0)
    for part in (LOW_UP, LOW_DOWN, HIGH_UP, HIGH_DOWN):
        narrow(mixed, part[0], me, *part)
        if part is LOW_UP:
            send(own, rest(LOW_UP), up)
        if part is LOW_DOWN:
            send(own, rest(LOW_DOWN), down)
            send(own, LOW_DOWN, up)
            send(own, LOW_UP, down)
        if part is HIGH_UP:
            send(own, rest(HIGH_UP), across)
            send(own, HIGH_UP, up)
    send(own, HIGH_DOWN, down, across, up)
    send(own, HIGH_UP, down)
    for part in (LOW_UP, LOW_DOWN, HIGH_UP, HIGH_DOWN):
        share(own, part, 0)
    for n, (block, (part, _)) in enumerate(zip((BELOW, ABOVE, SIDE), early_parts)):
        wait_bytes(early.at[n], early_recv.at[n])
        narrow(early.at[n], 0, device(*block), part[0], EARLY)

    arrived(0)
    send(BELOW, LOW_UP, up)
    send(ABOVE, LOW_DOWN, down)
    for j in range(1, PEERS):

        @pl.when(place + j < PEERS)
        def _():
            row_copy(place + j, place).wait_recv()
            row_copy(place, place + j).start()

    send(own, LOW_UP, across)
    send(own, LOW_DOWN, across)
    for block, part in ((BELOW, LOW_UP), (ABOVE, LOW_DOWN)):
        send(block, part, across)
        share(block, part)
    arrived(1)
    send(SIDE, HIGH_UP, up)
    share(SIDE, HIGH_UP)
    arrived(2)
    for block, part in ARRIVALS[2]:
        send(block, part, across)
        share(block, part)
    arrived(3)
    send(SIDE, HIGH_DOWN, down, up)
    send(SIDE, HIGH_UP, down)
    share(SIDE, HIGH_DOWN)
    arrived(4)
    send(BELOW, HIGH_UP, up)
    send(ABOVE, HIGH_DOWN, down)
    for block, part in ARRIVALS[4]:
        share(block, part)
    for j in range(1, PEERS):

        @pl.when(place + j >= PEERS)
        def _():
            row_copy(place + j - PEERS, place).wait_recv()

    flat = lax.broadcasted_iota(jnp.int32, (8, LANES), 0) * LANES + lax.broadcasted_iota(
        jnp.int32, (8, LANES), 1
    )
    image = jnp.zeros((8, LANES), jnp.float32)
    for j in range(PEERS):
        first = (core * PEERS + j) * NORM
        gains = pltpu.roll(jnp.broadcast_to(norm_rows[j], (8, LANES)), lax.rem(first, LANES), 1)
        image = jnp.where((flat >= first) & (flat < first + NORM), gains, image)
    norm_images[core, chip] = image.astype(jnp.bfloat16)
    for dz, dy in others:
        remote(
            norm_images.at[core, chip], image_sem.at[0], image_sem.at[1], rows=device(dz, dy)
        ).start()

    arrived(5)
    for block, part in ARRIVALS[5]:
        share(block, part, 0)

    def lend(parts, line, lent):
        @pl.when(core == 1)
        def _():
            for block, part, target in parts:
                there = ((block[0] - target[0]) % 2, (block[1] - target[1]) % 4)
                assert line_of[there, part] == line
                start(device(*block), part, 2, recv_sem.at[line], device(*target))
            wait_rows(lent[1], sibling_sem.at[lent[0]])
            for block, part, target in parts:
                recv = recv_sem.at[line - OWN_LENT + SIBLING_LENT]
                start(device(*block, 1), part, 2, recv, device(*target))

        @pl.when(core == 0)
        def _():
            wait_rows(lent[1], sibling_sem.at[lent[0]])

    arrived(6)
    send(FAR, LOW_UP, across)
    for part in LAST_ACROSS:
        send(FAR, part, across)
    share(FAR, LOW_DOWN, 3)
    share(FAR, LOW_UP)
    arrived(7)
    for part in LAST_UP:
        send(SIDE_BELOW, part, up)
    for part in LAST_DOWN:
        send(SIDE_ABOVE, part, down)
    share(SIDE_BELOW, HIGH_UP, 2)
    share(SIDE_ABOVE, HIGH_DOWN, 2)
    lend(((FAR, LENT_ACROSS, across),), OWN_LENT + 1, (3, LOW_DOWN[1]))
    lend(
        ((SIDE_BELOW, LENT_UP, up), (SIDE_ABOVE, LENT_DOWN, down)),
        OWN_LENT,
        (2, HIGH_UP[1] + HIGH_DOWN[1]),
    )
    arrived(8)
    for block, part in ARRIVALS[8]:
        share(block, part)
    wait_bytes(norm_images.at[0, pl.ds(0, CHIPS - 1)], image_sem.at[1])
    remote(norm_images.at[core], both_sem.at[0], both_sem.at[1], rows=device(0, 0, 1)).start()
    for line in range(9, OWN_LENT):
        arrived(line)
        for block, part in ARRIVALS[line]:
            share(block, part)

    @pl.when(core == 1)
    def _():
        for line in range(OWN_LENT, len(ARRIVALS)):
            arrived(line)
            for block, part in ARRIVALS[line]:
                start(device(*block), part, 2, sibling_sem.at[1], device(0, 0, 1))
            rows = sum(part[1] for _, part in ARRIVALS[line])
            wait_rows(rows, recv_sem.at[line - OWN_LENT + SIBLING_LENT])
            for block, part in ARRIVALS[line]:
                start(device(*block, 1), part, 2, sibling_sem.at[1], device(0, 0, 1))

    wait_bytes(norm_images.at[0], both_sem.at[1])
    for j in range(CHIPS):
        norm_all[pl.ds(7 * j, 8), :] = norm_images[0, j].astype(jnp.float32) + norm_images[
            1, j
        ].astype(jnp.float32)
    serve[...] = norm_all[pl.ds(0, NORM), :].astype(serve.dtype)
    wait_bytes(sums.at[pl.ds(0, CHIPS - 1)], sum_sem.at[0])
    wait_bytes(halves.at[0], half_sem.at[0])
    wait_bytes(norm_rows.at[pl.ds(0, PEERS - 1)], row_send.at[0])
    wait_bytes(norm_images.at[0, pl.ds(0, CHIPS - 1)], image_sem.at[0])
    wait_bytes(norm_images.at[0], both_sem.at[0])
    wait_bytes(early, early_send.at[0])
    wait_rows(2 * depth, sibling_sem.at[0])
    lent = LENT_UP[1] + LENT_DOWN[1] + LENT_ACROSS[1]
    other_rows = rows_sent[1] - 2 * depth - LOW_DOWN[1] - HIGH_UP[1] - HIGH_DOWN[1]

    @pl.when(core == 0)
    def _():
        wait_rows(other_rows + 2 * lent, sibling_sem.at[1])

    @pl.when(core == 1)
    def _():
        wait_rows(other_rows, sibling_sem.at[1])
        wait_rows(rows_sent[2], send_sem.at[2])

    assert rows_sent[2] == 4 * lent and rows_sent[1] + lent == DEVICES // 2 * depth
    wait_rows(rows_sent[0], send_sem.at[0])
    wait_rows(rows_sent[1], send_sem.at[1])


def write_kernel(
    blocks,
    scale_query,
    scale_key,
    scale_value,
    serve,
    query,
    key,
    value,
    query_scale,
    key_scale,
    value_scale,
    gains,
    sem,
    small_sem,
):
    depth = blocks.shape[1]
    outs = (query, key, value)
    for b in range(DEVICES):
        at = 0
        for n, out in enumerate(outs):
            pltpu.make_async_copy(
                blocks.at[b, :, pl.ds(at, out.shape[1])],
                out.at[pl.ds(b * depth, depth), :],
                sem.at[n],
            ).start()
            at += out.shape[1]
    small = (
        (scale_query, query_scale),
        (scale_key, key_scale),
        (scale_value, value_scale),
        (serve, gains),
    )
    for i, (source, target) in enumerate(small):
        pltpu.make_async_copy(source, target, small_sem.at[i]).start()
    for n, out in enumerate(outs):
        pltpu.make_async_copy(out, out, sem.at[n]).wait()
    for i, (source, target) in enumerate(small):
        pltpu.make_async_copy(source, target, small_sem.at[i]).wait()


def shards(
    one_query,
    other_query,
    one_key,
    other_key,
    one_value,
    other_value,
    mix_share,
    norm_train,
    norm_step,
):
    f32, bf16 = jnp.float32, jnp.bfloat16
    depth, queries = one_query.shape
    keys = one_key.shape[1]
    wide = queries + 2 * keys
    tall = -(-depth // LANES) * LANES
    dma = pltpu.SemaphoreType.DMA
    hbm, vmem = pl.BlockSpec(memory_space=pltpu.HBM), pl.BlockSpec(memory_space=pltpu.VMEM)
    blocks, scale_query, scale_key, scale_value, serve = pl.pallas_call(
        gather_kernel,
        out_shape=(
            pltpu.VMEM((DEVICES, depth, wide), bf16),
            pltpu.VMEM((queries // LANES, LANES), f32),
            pltpu.VMEM((keys // LANES, LANES), f32),
            pltpu.VMEM((keys // LANES, LANES), f32),
            pltpu.VMEM((NORM, LANES), bf16),
        ),
        in_specs=[hbm] * 9,
        out_specs=[vmem] * 5,
        scratch_shapes=[
            pltpu.VMEM((2, depth, wide), f32),
            pltpu.VMEM((depth, wide), f32),
            pltpu.VMEM((tall, LANES), f32),
            pltpu.VMEM((1, tall), f32),
            pltpu.VMEM((1, depth), f32),
            pltpu.VMEM((1, NORM), f32),
            pltpu.VMEM((1, NORM), f32),
            pltpu.VMEM((CHIPS, 1, wide), f32),
            pltpu.VMEM((2, 1, wide), f32),
            pltpu.VMEM((PEERS, 1, LANES), f32),
            pltpu.VMEM((2, CHIPS, 8, LANES), bf16),
            pltpu.VMEM((64, LANES), f32),
            pltpu.VMEM((3, EARLY, wide), f32),
            dma((LOADS,)),
            dma((3,)),
            dma((3,)),
            dma((len(ARRIVALS) + 2,)),
            dma((4,)),
            dma((2,)),
            dma((2,)),
            dma((1,)),
            dma((PEERS,)),
            dma((2,)),
            dma((2,)),
            dma((1,)),
            dma((3,)),
        ],
        compiler_params=pltpu.CompilerParams(
            collective_id=0, has_side_effects=True, vmem_limit_bytes=48 * 1024 * 1024
        ),
        name="gather",
    )(
        one_query,
        other_query,
        one_key,
        other_key,
        one_value,
        other_value,
        mix_share.reshape(1, depth),
        norm_train.reshape(1, NORM),
        norm_step.reshape(1, NORM),
    )
    finals = pl.pallas_call(
        write_kernel,
        out_shape=(
            jax.ShapeDtypeStruct((DEVICES * depth, queries), bf16),
            jax.ShapeDtypeStruct((DEVICES * depth, keys), bf16),
            jax.ShapeDtypeStruct((DEVICES * depth, keys), bf16),
            jax.ShapeDtypeStruct((queries // LANES, LANES), f32),
            jax.ShapeDtypeStruct((keys // LANES, LANES), f32),
            jax.ShapeDtypeStruct((keys // LANES, LANES), f32),
            jax.ShapeDtypeStruct((NORM, LANES), bf16),
        ),
        in_specs=[vmem] * 5,
        out_specs=[hbm] * 7,
        scratch_shapes=[dma((3,)), dma((4,))],
        compiler_params=pltpu.CompilerParams(vmem_limit_bytes=1024 * 1024),
        name="write",
    )(blocks, scale_query, scale_key, scale_value, serve)
    return finals[:3] + tuple(a.reshape(-1) for a in finals[3:])


def solution(mesh):
    in_specs = (
        P("rows", "width"),
        P("rows", "width"),
        P("rows", "width"),
        P("rows", "width"),
        P("rows", "width"),
        P("rows", "width"),
        P("rows"),
        P(("rows", "width")),
        P(("rows", "width")),
    )
    out_specs = (
        P(None, "width"),
        P(None, "width"),
        P(None, "width"),
        P("width"),
        P("width"),
        P("width"),
        P(),
    )
    return jax.shard_map(shards, mesh=mesh, in_specs=in_specs, out_specs=out_specs, check_vma=False)
```

```python
import jax
import jax.numpy as jnp
from jax import lax
from jax.experimental import pallas as pl
from jax.experimental.pallas import tpu as pltpu
from jax.sharding import PartitionSpec as P

MESH = pl.DeviceIdType.MESH
LANES = 128
DEVICES = 16
CHIPS = 8
PEERS = 8
NORM = 56

LOW_UP, LOW_DOWN, HIGH_UP, HIGH_DOWN = (0, 104), (104, 96), (200, 120), (320, 128)
EARLY = 48
LAST_UP = ((200, 40), (240, 48), (288, 16))
LAST_DOWN = ((320, 64), (384, 32), (416, 16))
LAST_ACROSS = ((104, 64), (168, 16))
LENT_UP, LENT_DOWN, LENT_ACROSS = (304, 16), (432, 16), (184, 16)


def rest(part):
    return part[0] + EARLY, part[1] - EARLY


BELOW, ABOVE, FAR = (0, 3), (0, 1), (0, 2)
SIDE, SIDE_BELOW, SIDE_ABOVE, SIDE_FAR = (1, 0), (1, 3), (1, 1), (1, 2)
ARRIVALS = (
    ((BELOW, rest(LOW_UP)), (ABOVE, rest(LOW_DOWN))),
    ((SIDE, rest(HIGH_UP)),),
    ((BELOW, LOW_DOWN), (ABOVE, LOW_UP)),
    ((SIDE, HIGH_DOWN),),
    ((BELOW, HIGH_UP), (ABOVE, HIGH_DOWN)),
    ((BELOW, HIGH_DOWN), (ABOVE, HIGH_UP), (SIDE, LOW_UP), (SIDE, LOW_DOWN)),
    ((FAR, LOW_UP), (FAR, LOW_DOWN)),
    ((SIDE_BELOW, HIGH_UP), (SIDE_ABOVE, HIGH_DOWN)),
    (
        (SIDE_BELOW, LOW_UP),
        (SIDE_BELOW, LOW_DOWN),
        (SIDE_BELOW, HIGH_DOWN),
        (SIDE_ABOVE, HIGH_UP),
    ),
    ((SIDE_ABOVE, LOW_UP), (SIDE_ABOVE, LOW_DOWN), (FAR, HIGH_UP), (FAR, HIGH_DOWN)),
    ((SIDE_FAR, LOW_UP),),
    ((SIDE_FAR, LAST_UP[0]), (SIDE_FAR, LAST_DOWN[0])),
    ((SIDE_FAR, LAST_UP[1]), (SIDE_FAR, LAST_DOWN[1])),
    ((SIDE_FAR, LAST_ACROSS[0]),),
    ((SIDE_FAR, LAST_UP[2]), (SIDE_FAR, LAST_DOWN[2])),
    ((SIDE_FAR, LAST_ACROSS[1]),),
    ((SIDE_FAR, LENT_UP), (SIDE_FAR, LENT_DOWN)),
    ((SIDE_FAR, LENT_ACROSS),),
)
OWN_LENT = len(ARRIVALS) - 2
SIBLING_LENT = len(ARRIVALS)
LOADS = 4


def gather_kernel(
    one_query,
    other_query,
    one_key,
    other_key,
    one_value,
    other_value,
    mix,
    train,
    step,
    blocks,
    scale_query,
    scale_key,
    scale_value,
    serve,
    both,
    mixed,
    shares,
    share_row,
    mix_here,
    train_here,
    step_here,
    sums,
    halves,
    norm_rows,
    norm_images,
    norm_all,
    early,
    load_sem,
    small_sem,
    send_sem,
    recv_sem,
    sibling_sem,
    sum_sem,
    half_sem,
    row_send,
    row_recv,
    image_sem,
    both_sem,
    early_send,
    early_recv,
):
    depth, wide = mixed.shape
    tiles = wide // LANES
    me = lax.axis_index("rows")
    place = lax.axis_index("width")
    core = lax.rem(me, 2)
    y = lax.rem(lax.div(me, 2), 4)
    z = lax.div(me, 8)
    chip = lax.div(me, 2)

    def device(dz, dy, other=0):
        return lax.rem(z + dz, 2) * 8 + lax.rem(y + dy, 4) * 2 + lax.rem(core + other, 2)

    def remote(ref, send, recv, **target):
        return pltpu.make_async_remote_copy(
            src_ref=ref,
            dst_ref=ref,
            send_sem=send,
            recv_sem=recv,
            device_id=target,
            device_id_type=MESH,
        )

    def wait_bytes(ref, sem):
        pltpu.make_async_copy(ref, ref, sem).wait()

    chunk = depth // LOADS

    def load(i):
        rows = pl.ds(i * chunk, chunk)
        at = 0
        for pair in ((one_query, other_query), (one_key, other_key), (one_value, other_value)):
            for n, source in enumerate(pair):
                columns = pl.ds(at, source.shape[1])
                pltpu.make_async_copy(
                    source.at[rows, :], both.at[n, rows, columns], load_sem.at[i]
                ).start()
            at += pair[0].shape[1]

    load(0)
    for i, (source, target) in enumerate(
        ((mix, mix_here), (train, train_here), (step, step_here))
    ):
        pltpu.make_async_copy(source, target, small_sem.at[i]).start()
    barrier = pltpu.get_barrier_semaphore()
    others = ((1, 2), (1, 1), (1, 3), (0, 2), (1, 0), (0, 1), (0, 3))
    for goal in [device(dz, dy) for dz, dy in others] + [device(0, 0, 1)]:
        pl.semaphore_signal(barrier, inc=1, device_id={"rows": goal}, device_id_type=MESH)
    for j in range(1, PEERS):

        @pl.when(place + j < PEERS)
        def _():
            pl.semaphore_signal(
                barrier, inc=1, device_id={"width": place + j}, device_id_type=MESH
            )

    for i in range(1, LOADS):
        load(i)

    for i, target in enumerate((mix_here, train_here, step_here)):
        wait_bytes(target, small_sem.at[i])

    share_row[...] = jnp.zeros_like(share_row)
    share_row[:, pl.ds(0, depth)] = mix_here[...]
    for i in range(shares.shape[0] // LANES):
        row = share_row[:, pl.ds(i * LANES, LANES)]
        shares[pl.ds(i * LANES, LANES), :] = jnp.broadcast_to(row, (LANES, LANES)).T

    norm_rows[place] = jnp.zeros((1, LANES), jnp.float32)
    norm_rows[place, :, pl.ds(0, NORM)] = train_here[...] + step_here[...]

    def mix_rows(strip, partial):
        rows = pl.ds(pl.multiple_of(strip * 8, 8), 8)
        share = shares[rows, :]
        rest = 1.0 - share
        found = []
        for t in range(tiles):
            lanes = pl.ds(t * LANES, LANES)
            value = share * both[0, rows, lanes] + rest * both[1, rows, lanes]
            mixed[rows, lanes] = value
            found.append(partial[t] + value * value)
        return tuple(found)

    partial = tuple(jnp.zeros((8, LANES), jnp.float32) for _ in range(tiles))
    for i in range(LOADS):
        wait_bytes(both.at[:, pl.ds(i * chunk, chunk), :], load_sem.at[i])
        partial = lax.fori_loop(i * chunk // 8, (i + 1) * chunk // 8, mix_rows, partial, unroll=2)
    for t in range(tiles):
        sums[chip, :, pl.ds(t * LANES, LANES)] = jnp.sum(partial[t], axis=0, keepdims=True)

    pl.semaphore_wait(barrier, CHIPS + place)

    for dz, dy in others:
        remote(sums.at[chip], sum_sem.at[0], sum_sem.at[1], rows=device(dz, dy)).start()

    def row_copy(source, target):
        return remote(norm_rows.at[source], row_send.at[0], row_recv.at[source], width=target)

    for j in range(1, PEERS):

        @pl.when(place + j >= PEERS)
        def _():
            row_copy(place, place + j - PEERS).start()

    up, down, across = (0, 1), (0, 3), (1, 0)
    early_parts = ((LOW_UP, up), (LOW_DOWN, down), (HIGH_UP, across))
    for n, (part, target) in enumerate(early_parts):
        pltpu.make_async_remote_copy(
            src_ref=mixed.at[pl.ds(part[0], EARLY), :],
            dst_ref=early.at[n],
            send_sem=early_send.at[0],
            recv_sem=early_recv.at[n],
            device_id={"rows": device(*target)},
            device_id_type=MESH,
        ).start()

    wait_bytes(sums.at[pl.ds(0, CHIPS - 1)], sum_sem.at[1])
    half = sums[0]
    for j in range(1, CHIPS):
        half = half + sums[j]
    halves[core] = half
    remote(halves.at[core], half_sem.at[0], half_sem.at[1], rows=device(0, 0, 1)).start()
    wait_bytes(halves.at[0], half_sem.at[1])
    total = halves[0] + halves[1]
    scale = jnp.sqrt(total)
    t = 0
    for out in (scale_query, scale_key, scale_value):
        for i in range(out.shape[0]):
            out[i : i + 1, :] = scale[:, t * LANES : (t + 1) * LANES]
            t += 1
    inverse = 1.0 / scale
    factors = [
        jnp.broadcast_to(inverse[:, t * LANES : (t + 1) * LANES], (8, LANES)) for t in range(tiles)
    ]

    def narrow(source, skip, block, start, count):
        def body(strip, carry):
            here = pl.ds(pl.multiple_of(skip + strip * 8, 8), 8)
            there = pl.ds(pl.multiple_of(start + strip * 8, 8), 8)
            for t in range(tiles):
                lanes = pl.ds(t * LANES, LANES)
                blocks[block, there, lanes] = (source[here, lanes] * factors[t]).astype(jnp.bfloat16)
            return carry

        lax.fori_loop(0, count // 8, body, 0, unroll=4)

    rows_sent = {}

    def start(source, part, send_by, recv, goal):
        remote(
            blocks.at[source, pl.ds(*part), :], send_sem.at[send_by], recv, rows=goal
        ).start()
        rows_sent[send_by] = rows_sent.get(send_by, 0) + part[1]

    line_of = {arrival: n for n, line in enumerate(ARRIVALS) for arrival in line}

    def send(block, part, *targets):
        for target in targets:
            line = line_of[((block[0] - target[0]) % 2, (block[1] - target[1]) % 4), part]
            start(device(*block), part, 0, recv_sem.at[line], device(*target))

    def share(block, part, recv=1):
        start(device(*block), part, 1, sibling_sem.at[recv], device(0, 0, 1))

    def wait_rows(count, sem):
        strips = count // 8
        n = next(n for n in range(1, DEVICES + 1) if strips % n == 0 and strips // n <= depth // 8)
        wait_bytes(blocks.at[pl.ds(0, n), pl.ds(0, strips // n * 8), :], sem)

    def arrived(line):
        wait_rows(sum(part[1] for _, part in ARRIVALS[line]), recv_sem.at[line])

    own = (0, 0)
    for part in (LOW_UP, LOW_DOWN, HIGH_UP, HIGH_DOWN):
        narrow(mixed, part[0], me, *part)
        if part is LOW_UP:
            send(own, rest(LOW_UP), up)
        if part is LOW_DOWN:
            send(own, rest(LOW_DOWN), down)
            send(own, LOW_DOWN, up)
            send(own, LOW_UP, down)
        if part is HIGH_UP:
            send(own, rest(HIGH_UP), across)
            send(own, HIGH_UP, up)
    send(own, HIGH_DOWN, down, across, up)
    send(own, HIGH_UP, down)
    for part in (LOW_UP, LOW_DOWN, HIGH_UP, HIGH_DOWN):
        share(own, part, 0)
    for n, (block, (part, _)) in enumerate(zip((BELOW, ABOVE, SIDE), early_parts)):
        wait_bytes(early.at[n], early_recv.at[n])
        narrow(early.at[n], 0, device(*block), part[0], EARLY)

    arrived(0)
    send(BELOW, LOW_UP, up)
    send(ABOVE, LOW_DOWN, down)
    for j in range(1, PEERS):

        @pl.when(place + j < PEERS)
        def _():
            row_copy(place + j, place).wait_recv()
            row_copy(place, place + j).start()

    send(own, LOW_UP, across)
    send(own, LOW_DOWN, across)
    for block, part in ((BELOW, LOW_UP), (ABOVE, LOW_DOWN)):
        send(block, part, across)
        share(block, part)
    arrived(1)
    send(SIDE, HIGH_UP, up)
    share(SIDE, HIGH_UP)
    arrived(2)
    for block, part in ARRIVALS[2]:
        send(block, part, across)
        share(block, part)
    arrived(3)
    send(SIDE, HIGH_DOWN, down, up)
    send(SIDE, HIGH_UP, down)
    share(SIDE, HIGH_DOWN)
    arrived(4)
    send(BELOW, HIGH_UP, up)
    send(ABOVE, HIGH_DOWN, down)
    for block, part in ARRIVALS[4]:
        share(block, part)
    for j in range(1, PEERS):

        @pl.when(place + j >= PEERS)
        def _():
            row_copy(place + j - PEERS, place).wait_recv()

    flat = lax.broadcasted_iota(jnp.int32, (8, LANES), 0) * LANES + lax.broadcasted_iota(
        jnp.int32, (8, LANES), 1
    )
    image = jnp.zeros((8, LANES), jnp.float32)
    for j in range(PEERS):
        first = (core * PEERS + j) * NORM
        gains = pltpu.roll(jnp.broadcast_to(norm_rows[j], (8, LANES)), lax.rem(first, LANES), 1)
        image = jnp.where((flat >= first) & (flat < first + NORM), gains, image)
    norm_images[core, chip] = image.astype(jnp.bfloat16)
    for dz, dy in others:
        remote(
            norm_images.at[core, chip], image_sem.at[0], image_sem.at[1], rows=device(dz, dy)
        ).start()

    arrived(5)
    for block, part in ARRIVALS[5]:
        share(block, part, 0)

    def lend(parts, line, lent):
        @pl.when(core == 1)
        def _():
            for block, part, target in parts:
                there = ((block[0] - target[0]) % 2, (block[1] - target[1]) % 4)
                assert line_of[there, part] == line
                start(device(*block), part, 2, recv_sem.at[line], device(*target))
            wait_rows(lent[1], sibling_sem.at[lent[0]])
            for block, part, target in parts:
                recv = recv_sem.at[line - OWN_LENT + SIBLING_LENT]
                start(device(*block, 1), part, 2, recv, device(*target))

        @pl.when(core == 0)
        def _():
            wait_rows(lent[1], sibling_sem.at[lent[0]])

    arrived(6)
    send(FAR, LOW_UP, across)
    for part in LAST_ACROSS:
        send(FAR, part, across)
    share(FAR, LOW_DOWN, 3)
    share(FAR, LOW_UP)
    arrived(7)
    for part in LAST_UP:
        send(SIDE_BELOW, part, up)
    for part in LAST_DOWN:
        send(SIDE_ABOVE, part, down)
    share(SIDE_BELOW, HIGH_UP, 2)
    share(SIDE_ABOVE, HIGH_DOWN, 2)
    lend(((FAR, LENT_ACROSS, across),), OWN_LENT + 1, (3, LOW_DOWN[1]))
    lend(
        ((SIDE_BELOW, LENT_UP, up), (SIDE_ABOVE, LENT_DOWN, down)),
        OWN_LENT,
        (2, HIGH_UP[1] + HIGH_DOWN[1]),
    )
    arrived(8)
    for block, part in ARRIVALS[8]:
        share(block, part)
    wait_bytes(norm_images.at[0, pl.ds(0, CHIPS - 1)], image_sem.at[1])
    remote(norm_images.at[core], both_sem.at[0], both_sem.at[1], rows=device(0, 0, 1)).start()
    for line in range(9, OWN_LENT):
        arrived(line)
        for block, part in ARRIVALS[line]:
            share(block, part)

    @pl.when(core == 1)
    def _():
        for line in range(OWN_LENT, len(ARRIVALS)):
            arrived(line)
            for block, part in ARRIVALS[line]:
                start(device(*block), part, 2, sibling_sem.at[1], device(0, 0, 1))
            rows = sum(part[1] for _, part in ARRIVALS[line])
            wait_rows(rows, recv_sem.at[line - OWN_LENT + SIBLING_LENT])
            for block, part in ARRIVALS[line]:
                start(device(*block, 1), part, 2, sibling_sem.at[1], device(0, 0, 1))

    wait_bytes(norm_images.at[0], both_sem.at[1])
    for j in range(CHIPS):
        norm_all[pl.ds(7 * j, 8), :] = norm_images[0, j].astype(jnp.float32) + norm_images[
            1, j
        ].astype(jnp.float32)
    serve[...] = norm_all[pl.ds(0, NORM), :].astype(serve.dtype)
    wait_bytes(sums.at[pl.ds(0, CHIPS - 1)], sum_sem.at[0])
    wait_bytes(halves.at[0], half_sem.at[0])
    wait_bytes(norm_rows.at[pl.ds(0, PEERS - 1)], row_send.at[0])
    wait_bytes(norm_images.at[0, pl.ds(0, CHIPS - 1)], image_sem.at[0])
    wait_bytes(norm_images.at[0], both_sem.at[0])
    wait_bytes(early, early_send.at[0])
    wait_rows(2 * depth, sibling_sem.at[0])
    lent = LENT_UP[1] + LENT_DOWN[1] + LENT_ACROSS[1]
    other_rows = rows_sent[1] - 2 * depth - LOW_DOWN[1] - HIGH_UP[1] - HIGH_DOWN[1]

    @pl.when(core == 0)
    def _():
        wait_rows(other_rows + 2 * lent, sibling_sem.at[1])

    @pl.when(core == 1)
    def _():
        wait_rows(other_rows, sibling_sem.at[1])
        wait_rows(rows_sent[2], send_sem.at[2])

    assert rows_sent[2] == 4 * lent and rows_sent[1] + lent == DEVICES // 2 * depth
    wait_rows(rows_sent[0], send_sem.at[0])
    wait_rows(rows_sent[1], send_sem.at[1])


def write_kernel(
    blocks,
    scale_query,
    scale_key,
    scale_value,
    serve,
    query,
    key,
    value,
    query_scale,
    key_scale,
    value_scale,
    gains,
    sem,
    small_sem,
):
    depth = blocks.shape[1]
    outs = (query, key, value)
    for b in range(DEVICES):
        at = 0
        for n, out in enumerate(outs):
            pltpu.make_async_copy(
                blocks.at[b, :, pl.ds(at, out.shape[1])],
                out.at[pl.ds(b * depth, depth), :],
                sem.at[n],
            ).start()
            at += out.shape[1]
    small = (
        (scale_query, query_scale),
        (scale_key, key_scale),
        (scale_value, value_scale),
        (serve, gains),
    )
    for i, (source, target) in enumerate(small):
        pltpu.make_async_copy(source, target, small_sem.at[i]).start()
    for n, out in enumerate(outs):
        pltpu.make_async_copy(out, out, sem.at[n]).wait()
    for i, (source, target) in enumerate(small):
        pltpu.make_async_copy(source, target, small_sem.at[i]).wait()


def shards(
    one_query,
    other_query,
    one_key,
    other_key,
    one_value,
    other_value,
    mix_share,
    norm_train,
    norm_step,
):
    f32, bf16 = jnp.float32, jnp.bfloat16
    depth, queries = one_query.shape
    keys = one_key.shape[1]
    wide = queries + 2 * keys
    tall = -(-depth // LANES) * LANES
    dma = pltpu.SemaphoreType.DMA
    hbm, vmem = pl.BlockSpec(memory_space=pltpu.HBM), pl.BlockSpec(memory_space=pltpu.VMEM)
    blocks, scale_query, scale_key, scale_value, serve = pl.pallas_call(
        gather_kernel,
        out_shape=(
            pltpu.VMEM((DEVICES, depth, wide), bf16),
            pltpu.VMEM((queries // LANES, LANES), f32),
            pltpu.VMEM((keys // LANES, LANES), f32),
            pltpu.VMEM((keys // LANES, LANES), f32),
            pltpu.VMEM((NORM, LANES), bf16),
        ),
        in_specs=[hbm] * 9,
        out_specs=[vmem] * 5,
        scratch_shapes=[
            pltpu.VMEM((2, depth, wide), f32),
            pltpu.VMEM((depth, wide), f32),
            pltpu.VMEM((tall, LANES), f32),
            pltpu.VMEM((1, tall), f32),
            pltpu.VMEM((1, depth), f32),
            pltpu.VMEM((1, NORM), f32),
            pltpu.VMEM((1, NORM), f32),
            pltpu.VMEM((CHIPS, 1, wide), f32),
            pltpu.VMEM((2, 1, wide), f32),
            pltpu.VMEM((PEERS, 1, LANES), f32),
            pltpu.VMEM((2, CHIPS, 8, LANES), bf16),
            pltpu.VMEM((64, LANES), f32),
            pltpu.VMEM((3, EARLY, wide), f32),
            dma((LOADS,)),
            dma((3,)),
            dma((3,)),
            dma((len(ARRIVALS) + 2,)),
            dma((4,)),
            dma((2,)),
            dma((2,)),
            dma((1,)),
            dma((PEERS,)),
            dma((2,)),
            dma((2,)),
            dma((1,)),
            dma((3,)),
        ],
        compiler_params=pltpu.CompilerParams(
            collective_id=0, has_side_effects=True, vmem_limit_bytes=48 * 1024 * 1024
        ),
        name="gather",
    )(
        one_query,
        other_query,
        one_key,
        other_key,
        one_value,
        other_value,
        mix_share.reshape(1, depth),
        norm_train.reshape(1, NORM),
        norm_step.reshape(1, NORM),
    )
    finals = pl.pallas_call(
        write_kernel,
        out_shape=(
            jax.ShapeDtypeStruct((DEVICES * depth, queries), bf16),
            jax.ShapeDtypeStruct((DEVICES * depth, keys), bf16),
            jax.ShapeDtypeStruct((DEVICES * depth, keys), bf16),
            jax.ShapeDtypeStruct((queries // LANES, LANES), f32),
            jax.ShapeDtypeStruct((keys // LANES, LANES), f32),
            jax.ShapeDtypeStruct((keys // LANES, LANES), f32),
            jax.ShapeDtypeStruct((NORM, LANES), bf16),
        ),
        in_specs=[vmem] * 5,
        out_specs=[hbm] * 7,
        scratch_shapes=[dma((3,)), dma((4,))],
        compiler_params=pltpu.CompilerParams(vmem_limit_bytes=1024 * 1024),
        name="write",
    )(blocks, scale_query, scale_key, scale_value, serve)
    return finals[:3] + tuple(a.reshape(-1) for a in finals[3:])


def solution(mesh):
    in_specs = (
        P("rows", "width"),
        P("rows", "width"),
        P("rows", "width"),
        P("rows", "width"),
        P("rows", "width"),
        P("rows", "width"),
        P("rows"),
        P(("rows", "width")),
        P(("rows", "width")),
    )
    out_specs = (
        P(None, "width"),
        P(None, "width"),
        P(None, "width"),
        P("width"),
        P("width"),
        P("width"),
        P(),
    )
    return jax.shard_map(shards, mesh=mesh, in_specs=in_specs, out_specs=out_specs, check_vma=False)
```

```python
import jax
import jax.numpy as jnp
from jax import lax
from jax.experimental import pallas as pl
from jax.experimental.pallas import tpu as pltpu
from jax.sharding import PartitionSpec as P

MESH = pl.DeviceIdType.MESH
LANES = 128
DEVICES = 16
CHIPS = 8
PEERS = 8
NORM = 56

LOW_UP, LOW_DOWN, HIGH_UP, HIGH_DOWN = (0, 104), (104, 96), (200, 120), (320, 128)
EARLY = 48
LAST_UP = ((200, 40), (240, 48), (288, 16))
LAST_DOWN = ((320, 64), (384, 32), (416, 16))
LAST_ACROSS = ((104, 64), (168, 16))
LENT_UP, LENT_DOWN, LENT_ACROSS = (304, 16), (432, 16), (184, 16)


def rest(part):
    return part[0] + EARLY, part[1] - EARLY


BELOW, ABOVE, FAR = (0, 3), (0, 1), (0, 2)
SIDE, SIDE_BELOW, SIDE_ABOVE, SIDE_FAR = (1, 0), (1, 3), (1, 1), (1, 2)
ARRIVALS = (
    ((BELOW, rest(LOW_UP)), (ABOVE, rest(LOW_DOWN))),
    ((SIDE, rest(HIGH_UP)),),
    ((BELOW, LOW_DOWN), (ABOVE, LOW_UP)),
    ((SIDE, HIGH_DOWN),),
    ((BELOW, HIGH_UP), (ABOVE, HIGH_DOWN)),
    ((BELOW, HIGH_DOWN), (ABOVE, HIGH_UP), (SIDE, LOW_UP), (SIDE, LOW_DOWN)),
    ((FAR, LOW_UP), (FAR, LOW_DOWN)),
    ((SIDE_BELOW, HIGH_UP), (SIDE_ABOVE, HIGH_DOWN)),
    (
        (SIDE_BELOW, LOW_UP),
        (SIDE_BELOW, LOW_DOWN),
        (SIDE_BELOW, HIGH_DOWN),
        (SIDE_ABOVE, HIGH_UP),
    ),
    ((SIDE_ABOVE, LOW_UP), (SIDE_ABOVE, LOW_DOWN), (FAR, HIGH_UP), (FAR, HIGH_DOWN)),
    ((SIDE_FAR, LOW_UP),),
    ((SIDE_FAR, LAST_UP[0]), (SIDE_FAR, LAST_DOWN[0])),
    ((SIDE_FAR, LAST_UP[1]), (SIDE_FAR, LAST_DOWN[1])),
    ((SIDE_FAR, LAST_ACROSS[0]),),
    ((SIDE_FAR, LAST_UP[2]), (SIDE_FAR, LAST_DOWN[2])),
    ((SIDE_FAR, LAST_ACROSS[1]),),
    ((SIDE_FAR, LENT_UP), (SIDE_FAR, LENT_DOWN)),
    ((SIDE_FAR, LENT_ACROSS),),
)
OWN_LENT = len(ARRIVALS) - 2
SIBLING_LENT = len(ARRIVALS)
LOADS = 4


def gather_kernel(
    one_query,
    other_query,
    one_key,
    other_key,
    one_value,
    other_value,
    mix,
    train,
    step,
    blocks,
    scale_query,
    scale_key,
    scale_value,
    serve,
    both,
    mixed,
    shares,
    share_row,
    mix_here,
    train_here,
    step_here,
    sums,
    halves,
    norm_rows,
    norm_images,
    norm_all,
    early,
    load_sem,
    small_sem,
    send_sem,
    recv_sem,
    sibling_sem,
    sum_sem,
    half_sem,
    row_send,
    row_recv,
    image_sem,
    both_sem,
    early_send,
    early_recv,
):
    depth, wide = mixed.shape
    tiles = wide // LANES
    me = lax.axis_index("rows")
    place = lax.axis_index("width")
    core = lax.rem(me, 2)
    y = lax.rem(lax.div(me, 2), 4)
    z = lax.div(me, 8)
    chip = lax.div(me, 2)

    def device(dz, dy, other=0):
        return lax.rem(z + dz, 2) * 8 + lax.rem(y + dy, 4) * 2 + lax.rem(core + other, 2)

    def remote(ref, send, recv, **target):
        return pltpu.make_async_remote_copy(
            src_ref=ref,
            dst_ref=ref,
            send_sem=send,
            recv_sem=recv,
            device_id=target,
            device_id_type=MESH,
        )

    def wait_bytes(ref, sem):
        pltpu.make_async_copy(ref, ref, sem).wait()

    chunk = depth // LOADS

    def load(i):
        rows = pl.ds(i * chunk, chunk)
        at = 0
        for pair in ((one_query, other_query), (one_key, other_key), (one_value, other_value)):
            for n, source in enumerate(pair):
                columns = pl.ds(at, source.shape[1])
                pltpu.make_async_copy(
                    source.at[rows, :], both.at[n, rows, columns], load_sem.at[i]
                ).start()
            at += pair[0].shape[1]

    load(0)
    for i, (source, target) in enumerate(
        ((mix, mix_here), (train, train_here), (step, step_here))
    ):
        pltpu.make_async_copy(source, target, small_sem.at[i]).start()
    barrier = pltpu.get_barrier_semaphore()
    others = ((1, 2), (1, 1), (1, 3), (0, 2), (1, 0), (0, 1), (0, 3))
    for goal in [device(dz, dy) for dz, dy in others] + [device(0, 0, 1)]:
        pl.semaphore_signal(barrier, inc=1, device_id={"rows": goal}, device_id_type=MESH)
    for j in range(1, PEERS):

        @pl.when(place + j < PEERS)
        def _():
            pl.semaphore_signal(
                barrier, inc=1, device_id={"width": place + j}, device_id_type=MESH
            )

    for i in range(1, LOADS):
        load(i)

    for i, target in enumerate((mix_here, train_here, step_here)):
        wait_bytes(target, small_sem.at[i])

    share_row[...] = jnp.zeros_like(share_row)
    share_row[:, pl.ds(0, depth)] = mix_here[...]
    for i in range(shares.shape[0] // LANES):
        row = share_row[:, pl.ds(i * LANES, LANES)]
        shares[pl.ds(i * LANES, LANES), :] = jnp.broadcast_to(row, (LANES, LANES)).T

    norm_rows[place] = jnp.zeros((1, LANES), jnp.float32)
    norm_rows[place, :, pl.ds(0, NORM)] = train_here[...] + step_here[...]

    def mix_rows(strip, partial):
        rows = pl.ds(pl.multiple_of(strip * 8, 8), 8)
        share = shares[rows, :]
        rest = 1.0 - share
        found = []
        for t in range(tiles):
            lanes = pl.ds(t * LANES, LANES)
            value = share * both[0, rows, lanes] + rest * both[1, rows, lanes]
            mixed[rows, lanes] = value
            found.append(partial[t] + value * value)
        return tuple(found)

    partial = tuple(jnp.zeros((8, LANES), jnp.float32) for _ in range(tiles))
    for i in range(LOADS):
        wait_bytes(both.at[:, pl.ds(i * chunk, chunk), :], load_sem.at[i])
        partial = lax.fori_loop(i * chunk // 8, (i + 1) * chunk // 8, mix_rows, partial, unroll=2)
    for t in range(tiles):
        sums[chip, :, pl.ds(t * LANES, LANES)] = jnp.sum(partial[t], axis=0, keepdims=True)

    pl.semaphore_wait(barrier, CHIPS + place)

    for dz, dy in others:
        remote(sums.at[chip], sum_sem.at[0], sum_sem.at[1], rows=device(dz, dy)).start()

    def row_copy(source, target, rising):
        return remote(norm_rows.at[source], row_send.at[0], row_recv.at[rising], width=target)

    for j in range(1, PEERS):

        @pl.when(place + j >= PEERS)
        def _():
            row_copy(place, place + j - PEERS, 0).start()

    up, down, across = (0, 1), (0, 3), (1, 0)
    early_parts = ((LOW_UP, up), (LOW_DOWN, down), (HIGH_UP, across))
    for n, (part, target) in enumerate(early_parts):
        pltpu.make_async_remote_copy(
            src_ref=mixed.at[pl.ds(part[0], EARLY), :],
            dst_ref=early.at[n],
            send_sem=early_send.at[0],
            recv_sem=early_recv.at[0],
            device_id={"rows": device(*target)},
            device_id_type=MESH,
        ).start()

    wait_bytes(sums.at[pl.ds(0, CHIPS - 1)], sum_sem.at[1])
    half = sums[0]
    for j in range(1, CHIPS):
        half = half + sums[j]
    halves[core] = half
    remote(halves.at[core], half_sem.at[0], half_sem.at[1], rows=device(0, 0, 1)).start()
    wait_bytes(halves.at[0], half_sem.at[1])
    total = halves[0] + halves[1]
    scale = jnp.sqrt(total)
    t = 0
    for out in (scale_query, scale_key, scale_value):
        for i in range(out.shape[0]):
            out[i : i + 1, :] = scale[:, t * LANES : (t + 1) * LANES]
            t += 1
    inverse = 1.0 / scale
    factors = [
        jnp.broadcast_to(inverse[:, t * LANES : (t + 1) * LANES], (8, LANES)) for t in range(tiles)
    ]

    def narrow(source, skip, block, start, count):
        def body(strip, carry):
            here = pl.ds(pl.multiple_of(skip + strip * 8, 8), 8)
            there = pl.ds(pl.multiple_of(start + strip * 8, 8), 8)
            for t in range(tiles):
                lanes = pl.ds(t * LANES, LANES)
                blocks[block, there, lanes] = (source[here, lanes] * factors[t]).astype(jnp.bfloat16)
            return carry

        lax.fori_loop(0, count // 8, body, 0, unroll=4)

    rows_sent = {}

    def start(source, part, send_by, recv, goal):
        remote(
            blocks.at[source, pl.ds(*part), :], send_sem.at[send_by], recv, rows=goal
        ).start()
        rows_sent[send_by] = rows_sent.get(send_by, 0) + part[1]

    line_of = {arrival: n for n, line in enumerate(ARRIVALS) for arrival in line}

    def send(block, part, *targets):
        for target in targets:
            line = line_of[((block[0] - target[0]) % 2, (block[1] - target[1]) % 4), part]
            start(device(*block), part, 0, recv_sem.at[line], device(*target))

    def share(block, part, recv=1):
        start(device(*block), part, 1, sibling_sem.at[recv], device(0, 0, 1))

    def wait_rows(count, sem):
        strips = count // 8
        n = next(n for n in range(1, DEVICES + 1) if strips % n == 0 and strips // n <= depth // 8)
        wait_bytes(blocks.at[pl.ds(0, n), pl.ds(0, strips // n * 8), :], sem)

    def arrived(line):
        wait_rows(sum(part[1] for _, part in ARRIVALS[line]), recv_sem.at[line])

    own = (0, 0)
    for part in (LOW_UP, LOW_DOWN, HIGH_UP, HIGH_DOWN):
        narrow(mixed, part[0], me, *part)
        if part is LOW_UP:
            send(own, rest(LOW_UP), up)
        if part is LOW_DOWN:
            send(own, rest(LOW_DOWN), down)
            send(own, LOW_DOWN, up)
            send(own, LOW_UP, down)
        if part is HIGH_UP:
            send(own, rest(HIGH_UP), across)
            send(own, HIGH_UP, up)
    send(own, HIGH_DOWN, down, across, up)
    send(own, HIGH_UP, down)
    for part in (LOW_UP, LOW_DOWN, HIGH_UP, HIGH_DOWN):
        share(own, part, 0)
    wait_bytes(early, early_recv.at[0])
    for n, (block, (part, _)) in enumerate(zip((BELOW, ABOVE, SIDE), early_parts)):
        narrow(early.at[n], 0, device(*block), part[0], EARLY)

    arrived(0)
    send(BELOW, LOW_UP, up)
    send(ABOVE, LOW_DOWN, down)
    for p in range(PEERS - 1):

        @pl.when(place == p)
        def _():
            wait_bytes(norm_rows.at[pl.ds(0, PEERS - 1 - p)], row_recv.at[0])

    for j in range(1, PEERS):

        @pl.when(place + j < PEERS)
        def _():
            row_copy(place, place + j, 1).start()

    send(own, LOW_UP, across)
    send(own, LOW_DOWN, across)
    for block, part in ((BELOW, LOW_UP), (ABOVE, LOW_DOWN)):
        send(block, part, across)
        share(block, part)
    arrived(1)
    send(SIDE, HIGH_UP, up)
    share(SIDE, HIGH_UP)
    arrived(2)
    for block, part in ARRIVALS[2]:
        send(block, part, across)
        share(block, part)
    arrived(3)
    send(SIDE, HIGH_DOWN, down, up)
    send(SIDE, HIGH_UP, down)
    share(SIDE, HIGH_DOWN)
    arrived(4)
    send(BELOW, HIGH_UP, up)
    send(ABOVE, HIGH_DOWN, down)
    for block, part in ARRIVALS[4]:
        share(block, part)
    for p in range(1, PEERS):

        @pl.when(place == p)
        def _():
            wait_bytes(norm_rows.at[pl.ds(0, p)], row_recv.at[1])

    flat = lax.broadcasted_iota(jnp.int32, (8, LANES), 0) * LANES + lax.broadcasted_iota(
        jnp.int32, (8, LANES), 1
    )
    image = jnp.zeros((8, LANES), jnp.float32)
    for j in range(PEERS):
        first = (core * PEERS + j) * NORM
        gains = pltpu.roll(jnp.broadcast_to(norm_rows[j], (8, LANES)), lax.rem(first, LANES), 1)
        image = jnp.where((flat >= first) & (flat < first + NORM), gains, image)
    norm_images[core, chip] = image.astype(jnp.bfloat16)
    for dz, dy in others:
        remote(
            norm_images.at[core, chip], image_sem.at[0], image_sem.at[1], rows=device(dz, dy)
        ).start()

    arrived(5)
    for block, part in ARRIVALS[5]:
        share(block, part, 0)

    def lend(parts, line, lent):
        @pl.when(core == 1)
        def _():
            for block, part, target in parts:
                there = ((block[0] - target[0]) % 2, (block[1] - target[1]) % 4)
                assert line_of[there, part] == line
                start(device(*block), part, 2, recv_sem.at[line], device(*target))
            wait_rows(lent[1], sibling_sem.at[lent[0]])
            for block, part, target in parts:
                recv = recv_sem.at[line - OWN_LENT + SIBLING_LENT]
                start(device(*block, 1), part, 2, recv, device(*target))

        @pl.when(core == 0)
        def _():
            wait_rows(lent[1], sibling_sem.at[lent[0]])

    arrived(6)
    send(FAR, LOW_UP, across)
    for part in LAST_ACROSS:
        send(FAR, part, across)
    share(FAR, LOW_DOWN, 3)
    share(FAR, LOW_UP)
    arrived(7)
    for part in LAST_UP:
        send(SIDE_BELOW, part, up)
    for part in LAST_DOWN:
        send(SIDE_ABOVE, part, down)
    share(SIDE_BELOW, HIGH_UP, 2)
    share(SIDE_ABOVE, HIGH_DOWN, 2)
    lend(((FAR, LENT_ACROSS, across),), OWN_LENT + 1, (3, LOW_DOWN[1]))
    lend(
        ((SIDE_BELOW, LENT_UP, up), (SIDE_ABOVE, LENT_DOWN, down)),
        OWN_LENT,
        (2, HIGH_UP[1] + HIGH_DOWN[1]),
    )
    arrived(8)
    for block, part in ARRIVALS[8]:
        share(block, part)
    wait_bytes(norm_images.at[0, pl.ds(0, CHIPS - 1)], image_sem.at[1])
    remote(norm_images.at[core], both_sem.at[0], both_sem.at[1], rows=device(0, 0, 1)).start()
    for line in range(9, OWN_LENT):
        arrived(line)
        for block, part in ARRIVALS[line]:
            share(block, part)

    @pl.when(core == 1)
    def _():
        for line in range(OWN_LENT, len(ARRIVALS)):
            arrived(line)
            for block, part in ARRIVALS[line]:
                start(device(*block), part, 2, sibling_sem.at[1], device(0, 0, 1))
            rows = sum(part[1] for _, part in ARRIVALS[line])
            wait_rows(rows, recv_sem.at[line - OWN_LENT + SIBLING_LENT])
            for block, part in ARRIVALS[line]:
                start(device(*block, 1), part, 2, sibling_sem.at[1], device(0, 0, 1))

    wait_bytes(norm_images.at[0], both_sem.at[1])
    for j in range(CHIPS):
        norm_all[pl.ds(7 * j, 8), :] = norm_images[0, j].astype(jnp.float32) + norm_images[
            1, j
        ].astype(jnp.float32)
    serve[...] = norm_all[pl.ds(0, NORM), :].astype(serve.dtype)
    wait_bytes(sums.at[pl.ds(0, CHIPS - 1)], sum_sem.at[0])
    wait_bytes(halves.at[0], half_sem.at[0])
    wait_bytes(norm_rows.at[pl.ds(0, PEERS - 1)], row_send.at[0])
    wait_bytes(norm_images.at[0, pl.ds(0, CHIPS - 1)], image_sem.at[0])
    wait_bytes(norm_images.at[0], both_sem.at[0])
    wait_bytes(early, early_send.at[0])
    wait_rows(2 * depth, sibling_sem.at[0])
    lent = LENT_UP[1] + LENT_DOWN[1] + LENT_ACROSS[1]
    other_rows = rows_sent[1] - 2 * depth - LOW_DOWN[1] - HIGH_UP[1] - HIGH_DOWN[1]

    @pl.when(core == 0)
    def _():
        wait_rows(other_rows + 2 * lent, sibling_sem.at[1])

    @pl.when(core == 1)
    def _():
        wait_rows(other_rows, sibling_sem.at[1])
        wait_rows(rows_sent[2], send_sem.at[2])

    assert rows_sent[2] == 4 * lent and rows_sent[1] + lent == DEVICES // 2 * depth
    wait_rows(rows_sent[0], send_sem.at[0])
    wait_rows(rows_sent[1], send_sem.at[1])


def write_kernel(
    blocks,
    scale_query,
    scale_key,
    scale_value,
    serve,
    query,
    key,
    value,
    query_scale,
    key_scale,
    value_scale,
    gains,
    sem,
    small_sem,
):
    depth = blocks.shape[1]
    outs = (query, key, value)
    for b in range(DEVICES):
        at = 0
        for n, out in enumerate(outs):
            pltpu.make_async_copy(
                blocks.at[b, :, pl.ds(at, out.shape[1])],
                out.at[pl.ds(b * depth, depth), :],
                sem.at[n],
            ).start()
            at += out.shape[1]
    small = (
        (scale_query, query_scale),
        (scale_key, key_scale),
        (scale_value, value_scale),
        (serve, gains),
    )
    for i, (source, target) in enumerate(small):
        pltpu.make_async_copy(source, target, small_sem.at[i]).start()
    for n, out in enumerate(outs):
        pltpu.make_async_copy(out, out, sem.at[n]).wait()
    for i, (source, target) in enumerate(small):
        pltpu.make_async_copy(source, target, small_sem.at[i]).wait()


def shards(
    one_query,
    other_query,
    one_key,
    other_key,
    one_value,
    other_value,
    mix_share,
    norm_train,
    norm_step,
):
    f32, bf16 = jnp.float32, jnp.bfloat16
    depth, queries = one_query.shape
    keys = one_key.shape[1]
    wide = queries + 2 * keys
    tall = -(-depth // LANES) * LANES
    dma = pltpu.SemaphoreType.DMA
    hbm, vmem = pl.BlockSpec(memory_space=pltpu.HBM), pl.BlockSpec(memory_space=pltpu.VMEM)
    blocks, scale_query, scale_key, scale_value, serve = pl.pallas_call(
        gather_kernel,
        out_shape=(
            pltpu.VMEM((DEVICES, depth, wide), bf16),
            pltpu.VMEM((queries // LANES, LANES), f32),
            pltpu.VMEM((keys // LANES, LANES), f32),
            pltpu.VMEM((keys // LANES, LANES), f32),
            pltpu.VMEM((NORM, LANES), bf16),
        ),
        in_specs=[hbm] * 9,
        out_specs=[vmem] * 5,
        scratch_shapes=[
            pltpu.VMEM((2, depth, wide), f32),
            pltpu.VMEM((depth, wide), f32),
            pltpu.VMEM((tall, LANES), f32),
            pltpu.VMEM((1, tall), f32),
            pltpu.VMEM((1, depth), f32),
            pltpu.VMEM((1, NORM), f32),
            pltpu.VMEM((1, NORM), f32),
            pltpu.VMEM((CHIPS, 1, wide), f32),
            pltpu.VMEM((2, 1, wide), f32),
            pltpu.VMEM((PEERS, 1, LANES), f32),
            pltpu.VMEM((2, CHIPS, 8, LANES), bf16),
            pltpu.VMEM((64, LANES), f32),
            pltpu.VMEM((3, EARLY, wide), f32),
            dma((LOADS,)),
            dma((3,)),
            dma((3,)),
            dma((len(ARRIVALS) + 2,)),
            dma((4,)),
            dma((2,)),
            dma((2,)),
            dma((1,)),
            dma((2,)),
            dma((2,)),
            dma((2,)),
            dma((1,)),
            dma((1,)),
        ],
        compiler_params=pltpu.CompilerParams(
            collective_id=0, has_side_effects=True, vmem_limit_bytes=48 * 1024 * 1024
        ),
        name="gather",
    )(
        one_query,
        other_query,
        one_key,
        other_key,
        one_value,
        other_value,
        mix_share.reshape(1, depth),
        norm_train.reshape(1, NORM),
        norm_step.reshape(1, NORM),
    )
    finals = pl.pallas_call(
        write_kernel,
        out_shape=(
            jax.ShapeDtypeStruct((DEVICES * depth, queries), bf16),
            jax.ShapeDtypeStruct((DEVICES * depth, keys), bf16),
            jax.ShapeDtypeStruct((DEVICES * depth, keys), bf16),
            jax.ShapeDtypeStruct((queries // LANES, LANES), f32),
            jax.ShapeDtypeStruct((keys // LANES, LANES), f32),
            jax.ShapeDtypeStruct((keys // LANES, LANES), f32),
            jax.ShapeDtypeStruct((NORM, LANES), bf16),
        ),
        in_specs=[vmem] * 5,
        out_specs=[hbm] * 7,
        scratch_shapes=[dma((3,)), dma((4,))],
        compiler_params=pltpu.CompilerParams(vmem_limit_bytes=1024 * 1024),
        name="write",
    )(blocks, scale_query, scale_key, scale_value, serve)
    return finals[:3] + tuple(a.reshape(-1) for a in finals[3:])


def solution(mesh):
    in_specs = (
        P("rows", "width"),
        P("rows", "width"),
        P("rows", "width"),
        P("rows", "width"),
        P("rows", "width"),
        P("rows", "width"),
        P("rows"),
        P(("rows", "width")),
        P(("rows", "width")),
    )
    out_specs = (
        P(None, "width"),
        P(None, "width"),
        P(None, "width"),
        P("width"),
        P("width"),
        P("width"),
        P(),
    )
    return jax.shard_map(shards, mesh=mesh, in_specs=in_specs, out_specs=out_specs, check_vma=False)
```

```python
import jax
import jax.numpy as jnp
from jax import lax
from jax.experimental import pallas as pl
from jax.experimental.pallas import tpu as pltpu
from jax.sharding import PartitionSpec as P

MESH = pl.DeviceIdType.MESH
LANES = 128
DEVICES = 16
CHIPS = 8
PEERS = 8
NORM = 56

LOW_UP, LOW_DOWN, HIGH_UP, HIGH_DOWN = (0, 104), (104, 96), (200, 120), (320, 128)
EARLY = 48
LAST_UP = ((200, 40), (240, 48), (288, 16))
LAST_DOWN = ((320, 64), (384, 32), (416, 16))
LAST_ACROSS = ((104, 64), (168, 16))
LENT_UP, LENT_DOWN, LENT_ACROSS = (304, 16), (432, 16), (184, 16)


def rest(part):
    return part[0] + EARLY, part[1] - EARLY


BELOW, ABOVE, FAR = (0, 3), (0, 1), (0, 2)
SIDE, SIDE_BELOW, SIDE_ABOVE, SIDE_FAR = (1, 0), (1, 3), (1, 1), (1, 2)
ARRIVALS = (
    ((BELOW, rest(LOW_UP)), (ABOVE, rest(LOW_DOWN))),
    ((SIDE, rest(HIGH_UP)),),
    ((BELOW, LOW_DOWN), (ABOVE, LOW_UP)),
    ((SIDE, HIGH_DOWN),),
    ((BELOW, HIGH_UP), (ABOVE, HIGH_DOWN)),
    ((BELOW, HIGH_DOWN), (ABOVE, HIGH_UP), (SIDE, LOW_UP), (SIDE, LOW_DOWN)),
    ((FAR, LOW_UP), (FAR, LOW_DOWN)),
    ((SIDE_BELOW, HIGH_UP), (SIDE_ABOVE, HIGH_DOWN)),
    (
        (SIDE_BELOW, LOW_UP),
        (SIDE_BELOW, LOW_DOWN),
        (SIDE_BELOW, HIGH_DOWN),
        (SIDE_ABOVE, HIGH_UP),
    ),
    ((SIDE_ABOVE, LOW_UP), (SIDE_ABOVE, LOW_DOWN), (FAR, HIGH_UP), (FAR, HIGH_DOWN)),
    ((SIDE_FAR, LOW_UP),),
    ((SIDE_FAR, LAST_UP[0]), (SIDE_FAR, LAST_DOWN[0])),
    ((SIDE_FAR, LAST_UP[1]), (SIDE_FAR, LAST_DOWN[1])),
    ((SIDE_FAR, LAST_ACROSS[0]),),
    ((SIDE_FAR, LAST_UP[2]), (SIDE_FAR, LAST_DOWN[2])),
    ((SIDE_FAR, LAST_ACROSS[1]),),
    ((SIDE_FAR, LENT_UP), (SIDE_FAR, LENT_DOWN)),
    ((SIDE_FAR, LENT_ACROSS),),
)
OWN_LENT = len(ARRIVALS) - 2
SIBLING_LENT = len(ARRIVALS)
LOADS = 7


def gather_kernel(
    one_query,
    other_query,
    one_key,
    other_key,
    one_value,
    other_value,
    mix,
    train,
    step,
    blocks,
    scale_query,
    scale_key,
    scale_value,
    serve,
    both,
    mixed,
    shares,
    share_row,
    mix_here,
    train_here,
    step_here,
    sums,
    halves,
    norm_rows,
    norm_images,
    norm_all,
    early,
    load_sem,
    small_sem,
    send_sem,
    recv_sem,
    sibling_sem,
    sum_sem,
    half_sem,
    row_send,
    row_recv,
    image_sem,
    both_sem,
    early_send,
    early_recv,
):
    depth, wide = mixed.shape
    tiles = wide // LANES
    me = lax.axis_index("rows")
    place = lax.axis_index("width")
    core = lax.rem(me, 2)
    y = lax.rem(lax.div(me, 2), 4)
    z = lax.div(me, 8)
    chip = lax.div(me, 2)

    def device(dz, dy, other=0):
        return lax.rem(z + dz, 2) * 8 + lax.rem(y + dy, 4) * 2 + lax.rem(core + other, 2)

    def remote(ref, send, recv, **target):
        return pltpu.make_async_remote_copy(
            src_ref=ref,
            dst_ref=ref,
            send_sem=send,
            recv_sem=recv,
            device_id=target,
            device_id_type=MESH,
        )

    def wait_bytes(ref, sem):
        pltpu.make_async_copy(ref, ref, sem).wait()

    chunk = depth // LOADS

    def load(i):
        rows = pl.ds(i * chunk, chunk)
        at = 0
        for pair in ((one_query, other_query), (one_key, other_key), (one_value, other_value)):
            for n, source in enumerate(pair):
                columns = pl.ds(at, source.shape[1])
                pltpu.make_async_copy(
                    source.at[rows, :], both.at[n, rows, columns], load_sem.at[i]
                ).start()
            at += pair[0].shape[1]

    load(0)
    for i, (source, target) in enumerate(
        ((mix, mix_here), (train, train_here), (step, step_here))
    ):
        pltpu.make_async_copy(source, target, small_sem.at[i]).start()
    barrier = pltpu.get_barrier_semaphore()
    others = ((1, 2), (1, 1), (1, 3), (0, 2), (1, 0), (0, 1), (0, 3))
    for goal in [device(dz, dy) for dz, dy in others] + [device(0, 0, 1)]:
        pl.semaphore_signal(barrier, inc=1, device_id={"rows": goal}, device_id_type=MESH)
    for j in range(1, PEERS):

        @pl.when(place + j < PEERS)
        def _():
            pl.semaphore_signal(
                barrier, inc=1, device_id={"width": place + j}, device_id_type=MESH
            )

    for i in range(1, LOADS):
        load(i)

    for i, target in enumerate((mix_here, train_here, step_here)):
        wait_bytes(target, small_sem.at[i])

    share_row[...] = jnp.zeros_like(share_row)
    share_row[:, pl.ds(0, depth)] = mix_here[...]
    for i in range(shares.shape[0] // LANES):
        row = share_row[:, pl.ds(i * LANES, LANES)]
        shares[pl.ds(i * LANES, LANES), :] = jnp.broadcast_to(row, (LANES, LANES)).T

    norm_rows[place] = jnp.zeros((1, LANES), jnp.float32)
    norm_rows[place, :, pl.ds(0, NORM)] = train_here[...] + step_here[...]

    def mix_rows(strip, partial):
        rows = pl.ds(pl.multiple_of(strip * 8, 8), 8)
        share = shares[rows, :]
        rest = 1.0 - share
        found = []
        for t in range(tiles):
            lanes = pl.ds(t * LANES, LANES)
            value = share * both[0, rows, lanes] + rest * both[1, rows, lanes]
            mixed[rows, lanes] = value
            found.append(partial[t] + value * value)
        return tuple(found)

    partial = tuple(jnp.zeros((8, LANES), jnp.float32) for _ in range(tiles))
    for i in range(LOADS):
        wait_bytes(both.at[:, pl.ds(i * chunk, chunk), :], load_sem.at[i])
        partial = lax.fori_loop(i * chunk // 8, (i + 1) * chunk // 8, mix_rows, partial, unroll=2)
    for t in range(tiles):
        sums[chip, :, pl.ds(t * LANES, LANES)] = jnp.sum(partial[t], axis=0, keepdims=True)

    pl.semaphore_wait(barrier, CHIPS + place)

    for dz, dy in others:
        remote(sums.at[chip], sum_sem.at[0], sum_sem.at[1], rows=device(dz, dy)).start()

    def row_copy(source, target):
        return remote(norm_rows.at[source], row_send.at[0], row_recv.at[source], width=target)

    for j in range(1, PEERS):

        @pl.when(place + j >= PEERS)
        def _():
            row_copy(place, place + j - PEERS).start()

    up, down, across = (0, 1), (0, 3), (1, 0)
    early_parts = ((LOW_UP, up), (LOW_DOWN, down), (HIGH_UP, across))
    for n, (part, target) in enumerate(early_parts):
        pltpu.make_async_remote_copy(
            src_ref=mixed.at[pl.ds(part[0], EARLY), :],
            dst_ref=early.at[n],
            send_sem=early_send.at[0],
            recv_sem=early_recv.at[n],
            device_id={"rows": device(*target)},
            device_id_type=MESH,
        ).start()

    wait_bytes(sums.at[pl.ds(0, CHIPS - 1)], sum_sem.at[1])
    half = sums[0]
    for j in range(1, CHIPS):
        half = half + sums[j]
    halves[core] = half
    remote(halves.at[core], half_sem.at[0], half_sem.at[1], rows=device(0, 0, 1)).start()
    wait_bytes(halves.at[0], half_sem.at[1])
    total = halves[0] + halves[1]
    scale = jnp.sqrt(total)
    t = 0
    for out in (scale_query, scale_key, scale_value):
        for i in range(out.shape[0]):
            out[i : i + 1, :] = scale[:, t * LANES : (t + 1) * LANES]
            t += 1
    inverse = 1.0 / scale
    factors = [
        jnp.broadcast_to(inverse[:, t * LANES : (t + 1) * LANES], (8, LANES)) for t in range(tiles)
    ]

    def narrow(source, skip, block, start, count):
        def body(strip, carry):
            here = pl.ds(pl.multiple_of(skip + strip * 8, 8), 8)
            there = pl.ds(pl.multiple_of(start + strip * 8, 8), 8)
            for t in range(tiles):
                lanes = pl.ds(t * LANES, LANES)
                blocks[block, there, lanes] = (source[here, lanes] * factors[t]).astype(jnp.bfloat16)
            return carry

        lax.fori_loop(0, count // 8, body, 0, unroll=4)

    rows_sent = {}

    def start(source, part, send_by, recv, goal):
        remote(
            blocks.at[source, pl.ds(*part), :], send_sem.at[send_by], recv, rows=goal
        ).start()
        rows_sent[send_by] = rows_sent.get(send_by, 0) + part[1]

    line_of = {arrival: n for n, line in enumerate(ARRIVALS) for arrival in line}

    def send(block, part, *targets):
        for target in targets:
            line = line_of[((block[0] - target[0]) % 2, (block[1] - target[1]) % 4), part]
            start(device(*block), part, 0, recv_sem.at[line], device(*target))

    def share(block, part, recv=1):
        start(device(*block), part, 1, sibling_sem.at[recv], device(0, 0, 1))

    def wait_rows(count, sem):
        strips = count // 8
        n = next(n for n in range(1, DEVICES + 1) if strips % n == 0 and strips // n <= depth // 8)
        wait_bytes(blocks.at[pl.ds(0, n), pl.ds(0, strips // n * 8), :], sem)

    def arrived(line):
        wait_rows(sum(part[1] for _, part in ARRIVALS[line]), recv_sem.at[line])

    own = (0, 0)
    for part in (LOW_UP, LOW_DOWN, HIGH_UP, HIGH_DOWN):
        narrow(mixed, part[0], me, *part)
        if part is LOW_UP:
            send(own, rest(LOW_UP), up)
        if part is LOW_DOWN:
            send(own, rest(LOW_DOWN), down)
            send(own, LOW_DOWN, up)
            send(own, LOW_UP, down)
        if part is HIGH_UP:
            send(own, rest(HIGH_UP), across)
            send(own, HIGH_UP, up)
    send(own, HIGH_DOWN, down, across, up)
    send(own, HIGH_UP, down)
    for part in (LOW_UP, LOW_DOWN, HIGH_UP, HIGH_DOWN):
        share(own, part, 0)
    for n, (block, (part, _)) in enumerate(zip((BELOW, ABOVE, SIDE), early_parts)):
        wait_bytes(early.at[n], early_recv.at[n])
        narrow(early.at[n], 0, device(*block), part[0], EARLY)

    arrived(0)
    send(BELOW, LOW_UP, up)
    send(ABOVE, LOW_DOWN, down)
    for j in range(1, PEERS):

        @pl.when(place + j < PEERS)
        def _():
            row_copy(place + j, place).wait_recv()
            row_copy(place, place + j).start()

    send(own, LOW_UP, across)
    send(own, LOW_DOWN, across)
    for block, part in ((BELOW, LOW_UP), (ABOVE, LOW_DOWN)):
        send(block, part, across)
        share(block, part)
    arrived(1)
    send(SIDE, HIGH_UP, up)
    share(SIDE, HIGH_UP)
    arrived(2)
    for block, part in ARRIVALS[2]:
        send(block, part, across)
        share(block, part)
    arrived(3)
    send(SIDE, HIGH_DOWN, down, up)
    send(SIDE, HIGH_UP, down)
    share(SIDE, HIGH_DOWN)
    arrived(4)
    send(BELOW, HIGH_UP, up)
    send(ABOVE, HIGH_DOWN, down)
    for block, part in ARRIVALS[4]:
        share(block, part)
    for j in range(1, PEERS):

        @pl.when(place + j >= PEERS)
        def _():
            row_copy(place + j - PEERS, place).wait_recv()

    flat = lax.broadcasted_iota(jnp.int32, (8, LANES), 0) * LANES + lax.broadcasted_iota(
        jnp.int32, (8, LANES), 1
    )
    image = jnp.zeros((8, LANES), jnp.float32)
    for j in range(PEERS):
        first = (core * PEERS + j) * NORM
        gains = pltpu.roll(jnp.broadcast_to(norm_rows[j], (8, LANES)), lax.rem(first, LANES), 1)
        image = jnp.where((flat >= first) & (flat < first + NORM), gains, image)
    norm_images[core, chip] = image.astype(jnp.bfloat16)
    for dz, dy in others:
        remote(
            norm_images.at[core, chip], image_sem.at[0], image_sem.at[1], rows=device(dz, dy)
        ).start()

    arrived(5)
    for block, part in ARRIVALS[5]:
        share(block, part, 0)

    def lend(parts, line, lent):
        @pl.when(core == 1)
        def _():
            for block, part, target in parts:
                there = ((block[0] - target[0]) % 2, (block[1] - target[1]) % 4)
                assert line_of[there, part] == line
                start(device(*block), part, 2, recv_sem.at[line], device(*target))
            wait_rows(lent[1], sibling_sem.at[lent[0]])
            for block, part, target in parts:
                recv = recv_sem.at[line - OWN_LENT + SIBLING_LENT]
                start(device(*block, 1), part, 2, recv, device(*target))

        @pl.when(core == 0)
        def _():
            wait_rows(lent[1], sibling_sem.at[lent[0]])

    arrived(6)
    send(FAR, LOW_UP, across)
    for part in LAST_ACROSS:
        send(FAR, part, across)
    share(FAR, LOW_DOWN, 3)
    share(FAR, LOW_UP)
    arrived(7)
    for part in LAST_UP:
        send(SIDE_BELOW, part, up)
    for part in LAST_DOWN:
        send(SIDE_ABOVE, part, down)
    share(SIDE_BELOW, HIGH_UP, 2)
    share(SIDE_ABOVE, HIGH_DOWN, 2)
    lend(((FAR, LENT_ACROSS, across),), OWN_LENT + 1, (3, LOW_DOWN[1]))
    lend(
        ((SIDE_BELOW, LENT_UP, up), (SIDE_ABOVE, LENT_DOWN, down)),
        OWN_LENT,
        (2, HIGH_UP[1] + HIGH_DOWN[1]),
    )
    arrived(8)
    for block, part in ARRIVALS[8]:
        share(block, part)
    wait_bytes(norm_images.at[0, pl.ds(0, CHIPS - 1)], image_sem.at[1])
    remote(norm_images.at[core], both_sem.at[0], both_sem.at[1], rows=device(0, 0, 1)).start()
    for line in range(9, OWN_LENT):
        arrived(line)
        for block, part in ARRIVALS[line]:
            share(block, part)

    @pl.when(core == 1)
    def _():
        for line in range(OWN_LENT, len(ARRIVALS)):
            arrived(line)
            for block, part in ARRIVALS[line]:
                start(device(*block), part, 2, sibling_sem.at[1], device(0, 0, 1))
            rows = sum(part[1] for _, part in ARRIVALS[line])
            wait_rows(rows, recv_sem.at[line - OWN_LENT + SIBLING_LENT])
            for block, part in ARRIVALS[line]:
                start(device(*block, 1), part, 2, sibling_sem.at[1], device(0, 0, 1))

    wait_bytes(norm_images.at[0], both_sem.at[1])
    for j in range(CHIPS):
        norm_all[pl.ds(7 * j, 8), :] = norm_images[0, j].astype(jnp.float32) + norm_images[
            1, j
        ].astype(jnp.float32)
    serve[...] = norm_all[pl.ds(0, NORM), :].astype(serve.dtype)
    wait_bytes(sums.at[pl.ds(0, CHIPS - 1)], sum_sem.at[0])
    wait_bytes(halves.at[0], half_sem.at[0])
    wait_bytes(norm_rows.at[pl.ds(0, PEERS - 1)], row_send.at[0])
    wait_bytes(norm_images.at[0, pl.ds(0, CHIPS - 1)], image_sem.at[0])
    wait_bytes(norm_images.at[0], both_sem.at[0])
    wait_bytes(early, early_send.at[0])
    wait_rows(2 * depth, sibling_sem.at[0])
    lent = LENT_UP[1] + LENT_DOWN[1] + LENT_ACROSS[1]
    other_rows = rows_sent[1] - 2 * depth - LOW_DOWN[1] - HIGH_UP[1] - HIGH_DOWN[1]

    @pl.when(core == 0)
    def _():
        wait_rows(other_rows + 2 * lent, sibling_sem.at[1])

    @pl.when(core == 1)
    def _():
        wait_rows(other_rows, sibling_sem.at[1])
        wait_rows(rows_sent[2], send_sem.at[2])

    assert rows_sent[2] == 4 * lent and rows_sent[1] + lent == DEVICES // 2 * depth
    wait_rows(rows_sent[0], send_sem.at[0])
    wait_rows(rows_sent[1], send_sem.at[1])


def write_kernel(
    blocks,
    scale_query,
    scale_key,
    scale_value,
    serve,
    query,
    key,
    value,
    query_scale,
    key_scale,
    value_scale,
    gains,
    sem,
    small_sem,
):
    depth = blocks.shape[1]
    outs = (query, key, value)
    quarter = depth // 4
    for b in range(DEVICES):
        for i in range(4):
            at = 0
            for n, out in enumerate(outs):
                pltpu.make_async_copy(
                    blocks.at[b, pl.ds(i * quarter, quarter), pl.ds(at, out.shape[1])],
                    out.at[pl.ds(b * depth + i * quarter, quarter), :],
                    sem.at[n],
                ).start()
                at += out.shape[1]
    small = (
        (scale_query, query_scale),
        (scale_key, key_scale),
        (scale_value, value_scale),
        (serve, gains),
    )
    for i, (source, target) in enumerate(small):
        pltpu.make_async_copy(source, target, small_sem.at[i]).start()
    for n, out in enumerate(outs):
        pltpu.make_async_copy(out, out, sem.at[n]).wait()
    for i, (source, target) in enumerate(small):
        pltpu.make_async_copy(source, target, small_sem.at[i]).wait()


def shards(
    one_query,
    other_query,
    one_key,
    other_key,
    one_value,
    other_value,
    mix_share,
    norm_train,
    norm_step,
):
    f32, bf16 = jnp.float32, jnp.bfloat16
    depth, queries = one_query.shape
    keys = one_key.shape[1]
    wide = queries + 2 * keys
    tall = -(-depth // LANES) * LANES
    dma = pltpu.SemaphoreType.DMA
    hbm, vmem = pl.BlockSpec(memory_space=pltpu.HBM), pl.BlockSpec(memory_space=pltpu.VMEM)
    blocks, scale_query, scale_key, scale_value, serve = pl.pallas_call(
        gather_kernel,
        out_shape=(
            pltpu.VMEM((DEVICES, depth, wide), bf16),
            pltpu.VMEM((queries // LANES, LANES), f32),
            pltpu.VMEM((keys // LANES, LANES), f32),
            pltpu.VMEM((keys // LANES, LANES), f32),
            pltpu.VMEM((NORM, LANES), bf16),
        ),
        in_specs=[hbm] * 9,
        out_specs=[vmem] * 5,
        scratch_shapes=[
            pltpu.VMEM((2, depth, wide), f32),
            pltpu.VMEM((depth, wide), f32),
            pltpu.VMEM((tall, LANES), f32),
            pltpu.VMEM((1, tall), f32),
            pltpu.VMEM((1, depth), f32),
            pltpu.VMEM((1, NORM), f32),
            pltpu.VMEM((1, NORM), f32),
            pltpu.VMEM((CHIPS, 1, wide), f32),
            pltpu.VMEM((2, 1, wide), f32),
            pltpu.VMEM((PEERS, 1, LANES), f32),
            pltpu.VMEM((2, CHIPS, 8, LANES), bf16),
            pltpu.VMEM((64, LANES), f32),
            pltpu.VMEM((3, EARLY, wide), f32),
            dma((LOADS,)),
            dma((3,)),
            dma((3,)),
            dma((len(ARRIVALS) + 2,)),
            dma((4,)),
            dma((2,)),
            dma((2,)),
            dma((1,)),
            dma((PEERS,)),
            dma((2,)),
            dma((2,)),
            dma((1,)),
            dma((3,)),
        ],
        compiler_params=pltpu.CompilerParams(
            collective_id=0, has_side_effects=True, vmem_limit_bytes=48 * 1024 * 1024
        ),
        name="gather",
    )(
        one_query,
        other_query,
        one_key,
        other_key,
        one_value,
        other_value,
        mix_share.reshape(1, depth),
        norm_train.reshape(1, NORM),
        norm_step.reshape(1, NORM),
    )
    finals = pl.pallas_call(
        write_kernel,
        out_shape=(
            jax.ShapeDtypeStruct((DEVICES * depth, queries), bf16),
            jax.ShapeDtypeStruct((DEVICES * depth, keys), bf16),
            jax.ShapeDtypeStruct((DEVICES * depth, keys), bf16),
            jax.ShapeDtypeStruct((queries // LANES, LANES), f32),
            jax.ShapeDtypeStruct((keys // LANES, LANES), f32),
            jax.ShapeDtypeStruct((keys // LANES, LANES), f32),
            jax.ShapeDtypeStruct((NORM, LANES), bf16),
        ),
        in_specs=[vmem] * 5,
        out_specs=[hbm] * 7,
        scratch_shapes=[dma((3,)), dma((4,))],
        compiler_params=pltpu.CompilerParams(vmem_limit_bytes=1024 * 1024),
        name="write",
    )(blocks, scale_query, scale_key, scale_value, serve)
    return finals[:3] + tuple(a.reshape(-1) for a in finals[3:])


def solution(mesh):
    in_specs = (
        P("rows", "width"),
        P("rows", "width"),
        P("rows", "width"),
        P("rows", "width"),
        P("rows", "width"),
        P("rows", "width"),
        P("rows"),
        P(("rows", "width")),
        P(("rows", "width")),
    )
    out_specs = (
        P(None, "width"),
        P(None, "width"),
        P(None, "width"),
        P("width"),
        P("width"),
        P("width"),
        P(),
    )
    return jax.shard_map(shards, mesh=mesh, in_specs=in_specs, out_specs=out_specs, check_vma=False)
```
